16 devices in a mesh: vp: 2 (over z), dp: 8 (over y, x, core).
Axes of the slice: x: 2, y: 2, z: 2, core: 2. Of those that a mesh axis runs over, the one named last changes fastest.
Arguments:
- student_x: bfloat16 [2560, 1536], P('dp')
- teacher_x: bfloat16 [512, 1536], P('dp')
- w_in: bfloat16 [1536, 2048], replicated
- b_in: bfloat16 [2048], replicated
- w_mid: bfloat16 [2048, 2048], replicated
- b_mid: bfloat16 [2048], replicated
- w_out: bfloat16 [2048, 256], replicated
- b_out: bfloat16 [256], replicated
- protos: bfloat16 [256, 65536], P(None, 'vp')
- ema_w_in: bfloat16 [1536, 2048], replicated
- ema_b_in: bfloat16 [2048], replicated
- ema_w_mid: bfloat16 [2048, 2048], replicated
- ema_b_mid: bfloat16 [2048], replicated
- ema_w_out: bfloat16 [2048, 256], replicated
- ema_b_out: bfloat16 [256], replicated
- ema_protos: bfloat16 [256, 65536], P(None, 'vp')
Outputs:
- output 1: float32 [], replicated
- output 2: float32 [1536, 2048], replicated
- output 3: float32 [2048], replicated
- output 4: float32 [2048, 2048], replicated
- output 5: float32 [2048], replicated
- output 6: float32 [2048, 256], replicated
- output 7: float32 [256], replicated
- output 8: float32 [256, 65536], P(None, 'vp')
All inputs are finite; a program needn't handle non-finite values.
Results may differ from the reference program's by a relative error of at most 0.00517659.
Values sent between devices are 32-bit elements.
A program may use at most 1 GiB of HBM per device.

```python
import jax
import jax.numpy as jnp
from jax import lax
from functools import partial

EMBED_DIM = 1536
HIDDEN_DIM = 2048
BOTTLENECK = 256
PROTOTYPES = 65536
TOTAL_IMAGES = 256
ALL_CROPS = 10
GLOBAL_CROPS = 2
SINK_ITERS = 3
IMAGE_BLOCK = 8
TEMP_STUDENT = 0.1
TEMP_TEACHER = 0.04


def setup_inputs(seed: int = 0) -> dict:
    keys = jax.random.split(jax.random.key(seed), 20)
    n_clusters = 4
    centers = jax.random.normal(keys[0], (n_clusters, EMBED_DIM), jnp.float32)
    cluster_of = (jnp.arange(TOTAL_IMAGES) * n_clusters) // TOTAL_IMAGES
    img_mean = centers[cluster_of] + 0.7 * jax.random.normal(keys[1], (TOTAL_IMAGES, EMBED_DIM), jnp.float32)
    teacher_x = img_mean[:, None, :] + 0.5 * jax.random.normal(keys[2], (TOTAL_IMAGES, GLOBAL_CROPS, EMBED_DIM), jnp.float32)
    student_x = img_mean[:, None, :] + 0.7 * jax.random.normal(keys[3], (TOTAL_IMAGES, ALL_CROPS, EMBED_DIM), jnp.float32)

    def make_dense(key, fan_in, fan_out):
        return jax.random.normal(key, (fan_in, fan_out), jnp.float32) * fan_in ** -0.5

    def make_bias(key, width):
        return 0.5 * jax.random.normal(key, (width,), jnp.float32)

    w_in = make_dense(keys[4], EMBED_DIM, HIDDEN_DIM)
    b_in = make_bias(keys[5], HIDDEN_DIM)
    w_mid = make_dense(keys[6], HIDDEN_DIM, HIDDEN_DIM)
    b_mid = make_bias(keys[7], HIDDEN_DIM)
    w_out = make_dense(keys[8], HIDDEN_DIM, BOTTLENECK)
    b_out = make_bias(keys[9], BOTTLENECK)
    col_scale = jnp.exp(0.5 * jax.random.normal(keys[10], (1, PROTOTYPES), jnp.float32))
    protos = jax.random.normal(keys[11], (BOTTLENECK, PROTOTYPES), jnp.float32) * col_scale
    ema_w_in = 0.8 * w_in + 0.6 * make_dense(keys[12], EMBED_DIM, HIDDEN_DIM)
    ema_b_in = 0.8 * b_in + 0.6 * make_bias(keys[13], HIDDEN_DIM)
    ema_w_mid = 0.8 * w_mid + 0.6 * make_dense(keys[14], HIDDEN_DIM, HIDDEN_DIM)
    ema_b_mid = 0.8 * b_mid + 0.6 * make_bias(keys[15], HIDDEN_DIM)
    ema_w_out = 0.8 * w_out + 0.6 * make_dense(keys[16], HIDDEN_DIM, BOTTLENECK)
    ema_b_out = 0.8 * b_out + 0.6 * make_bias(keys[17], BOTTLENECK)
    ema_protos = 0.8 * protos + 0.6 * jax.random.normal(keys[18], (BOTTLENECK, PROTOTYPES), jnp.float32) * col_scale
    return {
        'student_x': student_x.reshape(TOTAL_IMAGES * ALL_CROPS, EMBED_DIM).astype(jnp.bfloat16),
        'teacher_x': teacher_x.reshape(TOTAL_IMAGES * GLOBAL_CROPS, EMBED_DIM).astype(jnp.bfloat16),
        'w_in': w_in.astype(jnp.bfloat16),
        'b_in': b_in.astype(jnp.bfloat16),
        'w_mid': w_mid.astype(jnp.bfloat16),
        'b_mid': b_mid.astype(jnp.bfloat16),
        'w_out': w_out.astype(jnp.bfloat16),
        'b_out': b_out.astype(jnp.bfloat16),
        'protos': protos.astype(jnp.bfloat16),
        'ema_w_in': ema_w_in.astype(jnp.bfloat16),
        'ema_b_in': ema_b_in.astype(jnp.bfloat16),
        'ema_w_mid': ema_w_mid.astype(jnp.bfloat16),
        'ema_b_mid': ema_b_mid.astype(jnp.bfloat16),
        'ema_w_out': ema_w_out.astype(jnp.bfloat16),
        'ema_b_out': ema_b_out.astype(jnp.bfloat16),
        'ema_protos': ema_protos.astype(jnp.bfloat16),
    }


def snap_bf16(vals):
    return vals.astype(jnp.bfloat16).astype(jnp.float32)


def head_mlp(feats, w_in, b_in, w_mid, b_mid, w_out, b_out):
    hid_one = snap_bf16(jax.nn.gelu(jnp.dot(feats, w_in, preferred_element_type=jnp.float32) + b_in, approximate=False))
    hid_two = snap_bf16(jax.nn.gelu(jnp.dot(hid_one, w_mid, preferred_element_type=jnp.float32) + b_mid, approximate=False))
    proj = jnp.dot(hid_two, w_out, preferred_element_type=jnp.float32) + b_out
    return snap_bf16(proj / jnp.sqrt(jnp.sum(proj * proj, axis=-1, keepdims=True)))


def col_normalize(protos):
    return snap_bf16(protos / jnp.sqrt(jnp.sum(protos * protos, axis=0, keepdims=True)))


def block_loss(q_blk, emb_blk, proto_mat):
    logits = jnp.dot(emb_blk, proto_mat, preferred_element_type=jnp.float32) / TEMP_STUDENT
    log_p = jax.nn.log_softmax(logits.reshape(IMAGE_BLOCK, ALL_CROPS, PROTOTYPES), axis=-1)
    cross = jnp.einsum('iak,ivk->iav', q_blk, log_p)
    pair_mask = (jnp.arange(GLOBAL_CROPS)[:, None] != jnp.arange(ALL_CROPS)[None, :]).astype(jnp.float32)
    return -jnp.sum(cross * pair_mask) / (TOTAL_IMAGES * GLOBAL_CROPS * (ALL_CROPS - 1))


def reference(student_x, teacher_x, w_in, b_in, w_mid, b_mid, w_out, b_out, protos,
              ema_w_in, ema_b_in, ema_w_mid, ema_b_mid, ema_w_out, ema_b_out, ema_protos):
    t_emb = head_mlp(teacher_x.astype(jnp.float32), ema_w_in.astype(jnp.float32), ema_b_in.astype(jnp.float32),
                     ema_w_mid.astype(jnp.float32), ema_b_mid.astype(jnp.float32),
                     ema_w_out.astype(jnp.float32), ema_b_out.astype(jnp.float32))
    t_logits = jnp.dot(t_emb, col_normalize(ema_protos.astype(jnp.float32)), preferred_element_type=jnp.float32)
    n_rows = GLOBAL_CROPS * TOTAL_IMAGES
    q_mat = jnp.exp(t_logits / TEMP_TEACHER)
    q_mat = q_mat / jnp.sum(q_mat)
    for _ in range(SINK_ITERS):
        q_mat = q_mat / jnp.sum(q_mat, axis=0, keepdims=True) / PROTOTYPES
        q_mat = q_mat / jnp.sum(q_mat, axis=1, keepdims=True) / n_rows
    q_mat = q_mat * n_rows
    n_blocks = TOTAL_IMAGES // IMAGE_BLOCK
    q_blocks = q_mat.reshape(n_blocks, IMAGE_BLOCK, GLOBAL_CROPS, PROTOTYPES)

    feats = student_x.astype(jnp.float32)
    student_params = (w_in.astype(jnp.float32), b_in.astype(jnp.float32), w_mid.astype(jnp.float32),
                      b_mid.astype(jnp.float32), w_out.astype(jnp.float32), b_out.astype(jnp.float32))

    def student_embed(params):
        return head_mlp(feats, params[0], params[1], params[2], params[3], params[4], params[5])

    s_emb, emb_vjp = jax.vjp(student_embed, student_params)
    proto_unit, proto_vjp = jax.vjp(col_normalize, protos.astype(jnp.float32))
    emb_blocks = s_emb.reshape(n_blocks, IMAGE_BLOCK * ALL_CROPS, BOTTLENECK)

    def scan_step(carry, blk):
        q_blk, emb_blk = blk
        part_loss, blk_vjp = jax.vjp(partial(block_loss, q_blk), emb_blk, proto_unit)
        g_emb_blk, g_unit_blk = blk_vjp(jnp.ones((), jnp.float32))
        return (carry[0] + part_loss, carry[1] + g_unit_blk), g_emb_blk

    init = (jnp.zeros((), jnp.float32), jnp.zeros((BOTTLENECK, PROTOTYPES), jnp.float32))
    (loss, g_unit), g_emb = lax.scan(scan_step, init, (q_blocks, emb_blocks))
    g_params = emb_vjp(g_emb.reshape(TOTAL_IMAGES * ALL_CROPS, BOTTLENECK))[0]
    g_protos = proto_vjp(g_unit)[0]
    return (loss, g_params[0], g_params[1], g_params[2], g_params[3], g_params[4], g_params[5], g_protos)
```

```python
import functools

import jax
import jax.numpy as jnp
from jax import lax
from jax.experimental import pallas as pl
from jax.experimental.pallas import tpu as pltpu
from jax.sharding import Mesh, PartitionSpec as P

ALL_CROPS = 10
GLOBAL_CROPS = 2
SINK_ITERS = 3
TEMP_STUDENT = 0.1
TEMP_TEACHER = 0.04


def gelu_slope(pre):
    cdf = 0.5 * (1.0 + lax.erf(pre * 0.7071067811865476))
    return cdf + pre * jnp.exp(-0.5 * pre * pre) * 0.3989422804014327


def mlp_forward(feats, w_in, b_in, w_mid, b_mid, w_out, b_out):
    pre_one = jnp.dot(feats, w_in, preferred_element_type=jnp.float32) + b_in.astype(jnp.float32)
    hid_one = jax.nn.gelu(pre_one, approximate=False).astype(jnp.bfloat16)
    pre_two = jnp.dot(hid_one, w_mid, preferred_element_type=jnp.float32) + b_mid.astype(jnp.float32)
    hid_two = jax.nn.gelu(pre_two, approximate=False).astype(jnp.bfloat16)
    proj = jnp.dot(hid_two, w_out, preferred_element_type=jnp.float32) + b_out.astype(jnp.float32)
    inv_norm = lax.rsqrt(jnp.sum(proj * proj, axis=-1, keepdims=True))
    unit = proj * inv_norm
    return unit.astype(jnp.bfloat16), (pre_one, hid_one, pre_two, hid_two, unit, inv_norm)


def mlp_project(feats, w_in, b_in, w_mid, b_mid, w_out, b_out):
    pre_one = jnp.dot(feats, w_in, preferred_element_type=jnp.float32) + b_in.astype(jnp.float32)
    hid_one = jax.nn.gelu(pre_one, approximate=False).astype(jnp.bfloat16)
    pre_two = jnp.dot(hid_one, w_mid, preferred_element_type=jnp.float32) + b_mid.astype(jnp.float32)
    hid_two = jax.nn.gelu(pre_two, approximate=False).astype(jnp.bfloat16)
    return jnp.dot(hid_two, w_out, preferred_element_type=jnp.float32) + b_out.astype(jnp.float32)


def mlp_backward(g_emb, feats, saved, w_mid, w_out):
    pre_one, hid_one, pre_two, hid_two, unit, inv_norm = saved
    g_proj = (g_emb - unit * jnp.sum(unit * g_emb, axis=-1, keepdims=True)) * inv_norm
    g_proj_lo = g_proj.astype(jnp.bfloat16)
    g_w_out = jnp.einsum('nh,nb->hb', hid_two, g_proj_lo, preferred_element_type=jnp.float32)
    g_hid_two = jnp.einsum('nb,hb->nh', g_proj_lo, w_out, preferred_element_type=jnp.float32)
    g_pre_two = g_hid_two.astype(jnp.bfloat16).astype(jnp.float32) * gelu_slope(pre_two)
    g_pre_two_lo = g_pre_two.astype(jnp.bfloat16)
    g_w_mid = jnp.einsum('ng,nh->gh', hid_one, g_pre_two_lo, preferred_element_type=jnp.float32)
    g_hid_one = jnp.einsum('nh,gh->ng', g_pre_two_lo, w_mid, preferred_element_type=jnp.float32)
    g_pre_one = g_hid_one.astype(jnp.bfloat16).astype(jnp.float32) * gelu_slope(pre_one)
    g_w_in = jnp.einsum('nf,nh->fh', feats, g_pre_one.astype(jnp.bfloat16), preferred_element_type=jnp.float32)
    return (g_w_in, jnp.sum(g_pre_one, axis=0), g_w_mid, jnp.sum(g_pre_two, axis=0), g_w_out, jnp.sum(g_proj, axis=0))


def col_normalize(protos):
    proto_f = protos.astype(jnp.float32)
    inv_col = lax.rsqrt(jnp.sum(proto_f * proto_f, axis=0, keepdims=True))
    unit = proto_f * inv_col
    return unit.astype(jnp.bfloat16), unit, inv_col


def col_normalize_backward(g_unit, unit, inv_col):
    return (g_unit - unit * jnp.sum(unit * g_unit, axis=0, keepdims=True)) * inv_col


def gather_rows(vals, axis_name):
    return lax.all_gather(vals.astype(jnp.float32), axis_name, axis=0, tiled=True)


def round_kernel(wide_ref, out_ref):
    out_ref[...] = wide_ref[...].astype(out_ref.dtype)


def round_rows(wide):
    rows, width = wide.shape
    block = pl.BlockSpec((rows // 4, width), lambda i: (i, 0))
    return pl.pallas_call(
        round_kernel, out_shape=jax.ShapeDtypeStruct((rows, width), jnp.bfloat16), grid=(4,),
        in_specs=[block], out_specs=block,
        cost_estimate=pl.CostEstimate(flops=rows * width, bytes_accessed=6 * rows * width, transcendentals=0))(wide)


def unit_rows(proj):
    return (proj * lax.rsqrt(jnp.sum(proj * proj, axis=-1, keepdims=True))).astype(jnp.bfloat16)


def view_major(rows, n_img, views):
    width = rows.shape[1]
    return rows.reshape(n_img, views, width).transpose(1, 0, 2).reshape(n_img * views, width)


LANES = 128
AXES = ('vp', 'y', 'x', 'core')


def my_place(sizes):
    flat = 0
    for name, size in zip(AXES, sizes):
        flat = flat * size + lax.axis_index(name)
    return flat


def place_of(flat, sizes):
    coords = []
    for size in reversed(sizes):
        coords.append(lax.rem(flat, size))
        flat = flat // size
    return tuple(reversed(coords))


def greet_all(sizes, n_dev):
    barrier = pltpu.get_barrier_semaphore()
    me = my_place(sizes)
    for step in range(1, n_dev):
        peer = lax.rem(me + step, n_dev)
        pl.semaphore_signal(barrier, inc=1, device_id=place_of(peer, sizes), device_id_type=pl.DeviceIdType.MESH)


def await_all(n_dev):
    pl.semaphore_wait(pltpu.get_barrier_semaphore(), n_dev - 1)


def exchange(send_ref, recv_ref, send_sem, recv_sem, sizes, n_dev):
    me = my_place(sizes)
    copies = []
    for step in range(1, n_dev):
        peer = lax.rem(me + step, n_dev)
        copy = pltpu.make_async_remote_copy(
            src_ref=send_ref, dst_ref=recv_ref.at[step], send_sem=send_sem.at[step], recv_sem=recv_sem.at[step],
            device_id=place_of(peer, sizes), device_id_type=pl.DeviceIdType.MESH)
        copy.start()
        copies.append(copy)
    for copy in copies:
        copy.wait()
    total = send_ref[...]
    for step in range(1, n_dev):
        total = total + recv_ref[step]
    return total


def eye_mask():
    rows = lax.broadcasted_iota(jnp.int32, (LANES, LANES), 0)
    cols = lax.broadcasted_iota(jnp.int32, (LANES, LANES), 1)
    return rows == cols


def to_lanes(column):
    return jnp.sum(jnp.where(eye_mask(), jnp.broadcast_to(column, (LANES, LANES)), 0.0), axis=0, keepdims=True)


def to_rows(line):
    return jnp.sum(jnp.where(eye_mask(), jnp.broadcast_to(line, (LANES, LANES)), 0.0), axis=1, keepdims=True)


def fold_lanes(tile):
    total = tile[:, :LANES]
    for start in range(LANES, tile.shape[1], LANES):
        total = total + tile[:, start:start + LANES]
    return total


def sink_kernel(sizes, n_proto, block, t_ref, v_ref, hi_ref, lo_ref, row_ref,
                exp_ref, col_ref, scale_ref, part_ref, send_ref, recv_ref, send_sem, recv_sem):
    n_dev = 1
    for size in sizes:
        n_dev *= size
    n_rows, width = exp_ref.shape
    groups = n_rows // LANES
    steps = width // block
    greet_all(sizes, n_dev)

    def fill(step, total):
        cols = pl.ds(pl.multiple_of(step * block, block), block)
        proto_f = v_ref[:, cols].astype(jnp.float32)
        unit = (proto_f * lax.rsqrt(jnp.sum(proto_f * proto_f, axis=0, keepdims=True))).astype(jnp.bfloat16)
        grown = jnp.exp(jnp.dot(t_ref[...], unit, preferred_element_type=jnp.float32) * (1.0 / TEMP_TEACHER))
        exp_ref[:, cols] = grown
        sums = jnp.sum(grown, axis=0, keepdims=True)
        return total + fold_lanes(sums)

    total = lax.fori_loop(0, steps, fill, jnp.zeros((1, LANES), jnp.float32))
    total = jnp.broadcast_to(jnp.sum(total, axis=1, keepdims=True), (1, LANES))
    scale_ref[...] = jnp.ones_like(scale_ref)
    await_all(n_dev)
    for it in range(SINK_ITERS):
        part_ref[...] = jnp.zeros_like(part_ref)

        lax.fori_loop(0, width // LANES, lambda s, c: sweep_at(s, c, exp_ref, scale_ref, col_ref, part_ref, n_proto), 0)
        for group in range(groups):
            rows = pl.ds(group * LANES, LANES)
            send_ref[it, group:group + 1, :] = to_lanes(jnp.sum(part_ref[rows, :], axis=1, keepdims=True))
        send_ref[it, groups:groups + 1, :] = total
        sums = exchange(send_ref.at[it], recv_ref.at[it], send_sem.at[it], recv_sem.at[it], sizes, n_dev)
        crop = sums[:groups]
        if it == 0:
            whole = sums[groups:groups + 1]
            crop = crop * (whole * (1.0 / whole))
        scale = 1.0 / (crop * n_rows)
        for group in range(groups):
            rows = pl.ds(group * LANES, LANES)
            scale_ref[rows, :] = jnp.broadcast_to(to_rows(scale[group:group + 1]), (LANES, LANES))
        if it == SINK_ITERS - 1:
            row_ref[...] = jnp.zeros_like(row_ref)
            row_ref[:groups, :] = crop * scale * n_rows

    def finish(step, carry):
        cols = pl.ds(pl.multiple_of(step * LANES, LANES), LANES)
        target = exp_ref[:, cols] * scale_ref[...] * col_ref[:, cols] * n_rows
        high = target.astype(jnp.bfloat16)
        hi_ref[:, cols] = high
        lo_ref[:, cols] = (target - high.astype(jnp.float32)).astype(jnp.bfloat16)
        return carry

    lax.fori_loop(0, width // LANES, finish, 0)


def sweep_at(step, carry, exp_ref, scale_ref, col_ref, part_ref, n_proto):
    cols = pl.ds(pl.multiple_of(step * LANES, LANES), LANES)
    grown = exp_ref[:, cols]
    col = 1.0 / (jnp.sum(grown * scale_ref[...], axis=0, keepdims=True) * n_proto)
    col_ref[:, cols] = col
    part_ref[...] += grown * col
    return carry


def sinkhorn(t_all, ema_own, sizes, n_proto):
    n_rows, depth = t_all.shape
    width = ema_own.shape[1]
    n_dev = 1
    for size in sizes:
        n_dev *= size
    vmem = pl.BlockSpec(memory_space=pltpu.VMEM)
    target = jax.ShapeDtypeStruct((n_rows, width), jnp.bfloat16)
    return pl.pallas_call(
        functools.partial(sink_kernel, sizes, n_proto, 512),
        out_shape=(target, target, jax.ShapeDtypeStruct((8, LANES), jnp.float32)),
        in_specs=[vmem] * 2, out_specs=(vmem,) * 3,
        scratch_shapes=[
            pltpu.VMEM((n_rows, width), jnp.float32), pltpu.VMEM((1, width), jnp.float32),
            pltpu.VMEM((n_rows, LANES), jnp.float32), pltpu.VMEM((n_rows, LANES), jnp.float32),
            pltpu.VMEM((SINK_ITERS, 8, LANES), jnp.float32), pltpu.VMEM((SINK_ITERS, n_dev, 8, LANES), jnp.float32),
            pltpu.SemaphoreType.DMA((SINK_ITERS, n_dev)), pltpu.SemaphoreType.DMA((SINK_ITERS, n_dev))],
        compiler_params=pltpu.CompilerParams(collective_id=0, has_side_effects=True, vmem_limit_bytes=40 << 20),
        cost_estimate=pl.CostEstimate(flops=20 * 10 ** 9, bytes_accessed=12 << 20, transcendentals=n_rows * width),
    )(t_all, ema_own)


def soft_kernel(rows, s_ref, v_ref, hi_ref, lo_ref, exp_ref, part_ref, exp_u_ref, hi_u_ref, lo_u_ref):
    @pl.when(pl.program_id(0) == 0)
    def _():
        part_ref[...] = jnp.zeros_like(part_ref)
        exp_u_ref[...] = jnp.zeros_like(exp_u_ref)
        hi_u_ref[...] = jnp.zeros_like(hi_u_ref)
        lo_u_ref[...] = jnp.zeros_like(lo_u_ref)

    proto_f = v_ref[...].astype(jnp.float32)
    unit = (proto_f * lax.rsqrt(jnp.sum(proto_f * proto_f, axis=0, keepdims=True))).astype(jnp.bfloat16)
    across = (((1,), (1,)), ((), ()))
    hi_u_ref[...] += lax.dot_general(hi_ref[...], unit, across, preferred_element_type=jnp.float32)
    lo_u_ref[...] += lax.dot_general(lo_ref[...], unit, across, preferred_element_type=jnp.float32)

    def one(step, carry):
        at = pl.ds(pl.multiple_of(step * rows, rows), rows)
        logits = jnp.dot(s_ref[at, :], unit, preferred_element_type=jnp.float32) * (1.0 / TEMP_STUDENT)
        grown = jnp.exp(logits)
        part_ref[at, :] += fold_lanes(grown)
        low = grown.astype(jnp.bfloat16)
        exp_ref[at, :] = low
        exp_u_ref[at, :] += lax.dot_general(low, unit, across, preferred_element_type=jnp.float32)
        return carry

    lax.fori_loop(0, s_ref.shape[0] // rows, one, 0)


def soft_pass(s_all, protos_own, hi, lo):
    n_student, depth = s_all.shape
    n_rows, width = hi.shape
    block = 512
    whole = lambda shape: pl.BlockSpec(shape, lambda k: (0, 0))
    cols = lambda height: pl.BlockSpec((height, block), lambda k: (0, k))
    wide = lambda height, span: jax.ShapeDtypeStruct((height, span), jnp.float32)
    return pl.pallas_call(
        functools.partial(soft_kernel, 640),
        grid=(width // block,),
        out_shape=(jax.ShapeDtypeStruct((n_student, width), jnp.bfloat16), wide(n_student, LANES),
                   wide(n_student, depth), wide(n_rows, depth), wide(n_rows, depth)),
        in_specs=[whole((n_student, depth)), cols(depth), cols(n_rows), cols(n_rows)],
        out_specs=(cols(n_student), whole((n_student, LANES)), whole((n_student, depth)),
                   whole((n_rows, depth)), whole((n_rows, depth))),
        compiler_params=pltpu.CompilerParams(dimension_semantics=('arbitrary',), vmem_limit_bytes=50 << 20),
        cost_estimate=pl.CostEstimate(flops=13 * 10 ** 9, bytes_accessed=35 << 20, transcendentals=n_student * width),
    )(s_all, protos_own, hi, lo)


def total_kernel(sizes, part_ref, out_ref, send_ref, recv_ref, send_sem, recv_sem):
    n_dev = 1
    for size in sizes:
        n_dev *= size
    greet_all(sizes, n_dev)
    send_ref[...] = jnp.zeros_like(send_ref)
    for group in range(part_ref.shape[0] // LANES):
        rows = pl.ds(group * LANES, LANES)
        send_ref[group:group + 1, :] = to_lanes(jnp.sum(part_ref[rows, :], axis=1, keepdims=True))
    await_all(n_dev)
    out_ref[...] = exchange(send_ref, recv_ref, send_sem, recv_sem, sizes, n_dev)


def total_rows(part, sizes):
    lines = -(-part.shape[0] // (8 * LANES)) * 8
    n_dev = 1
    for size in sizes:
        n_dev *= size
    vmem = pl.BlockSpec(memory_space=pltpu.VMEM)
    return pl.pallas_call(
        functools.partial(total_kernel, sizes),
        out_shape=jax.ShapeDtypeStruct((lines, LANES), jnp.float32), in_specs=[vmem], out_specs=vmem,
        scratch_shapes=[
            pltpu.VMEM((lines, LANES), jnp.float32), pltpu.VMEM((n_dev, lines, LANES), jnp.float32),
            pltpu.SemaphoreType.DMA((n_dev,)), pltpu.SemaphoreType.DMA((n_dev,))],
        compiler_params=pltpu.CompilerParams(collective_id=1, has_side_effects=True),
        cost_estimate=pl.CostEstimate(flops=10 ** 9, bytes_accessed=2 << 20, transcendentals=0),
    )(part)


def grad_kernel(factor, soft_ref, pair_ref, exp_ref, hi_ref, v_ref, out_ref):
    g_unit = jnp.dot(soft_ref[...], exp_ref[...], preferred_element_type=jnp.float32)
    g_unit = (g_unit - jnp.dot(pair_ref[...], hi_ref[...], preferred_element_type=jnp.float32)) * factor
    proto_f = v_ref[...].astype(jnp.float32)
    inv_col = lax.rsqrt(jnp.sum(proto_f * proto_f, axis=0, keepdims=True))
    unit = proto_f * inv_col
    out_ref[...] = (g_unit - unit * jnp.sum(unit * g_unit, axis=0, keepdims=True)) * inv_col


def grad_pass(soft, pair, exp_lo, hi, protos_own, factor):
    depth, n_student = soft.shape
    n_rows, width = hi.shape
    block = 512
    whole = lambda shape: pl.BlockSpec(shape, lambda k: (0, 0))
    cols = lambda height: pl.BlockSpec((height, block), lambda k: (0, k))
    return pl.pallas_call(
        functools.partial(grad_kernel, factor), grid=(width // block,),
        out_shape=jax.ShapeDtypeStruct((depth, width), jnp.float32),
        in_specs=[whole((depth, n_student)), whole((depth, n_rows)), cols(n_student), cols(n_rows), cols(depth)],
        out_specs=cols(depth),
        compiler_params=pltpu.CompilerParams(dimension_semantics=('arbitrary',), vmem_limit_bytes=40 << 20),
        cost_estimate=pl.CostEstimate(flops=7 * 10 ** 9, bytes_accessed=33 << 20, transcendentals=0),
    )(soft, pair, exp_lo, hi, protos_own)


def crop_counts():
    crop_idx = jnp.arange(ALL_CROPS)
    return (GLOBAL_CROPS - (crop_idx < GLOBAL_CROPS).astype(jnp.int32)).astype(jnp.float32)


def solution(mesh):
    vp_size = mesh.shape['vp']
    dp_size = mesh.shape['dp']
    sizes = (vp_size, dp_size // 4, 2, 2)
    fine = Mesh(mesh.devices.reshape(sizes), AXES)
    data = ('y', 'x', 'core')

    def local_step(student_x, teacher_x, w_in, b_in, w_mid, b_mid, w_out, b_out, protos,
                   ema_w_in, ema_b_in, ema_w_mid, ema_b_mid, ema_w_out, ema_b_out, ema_protos):
        n_img = student_x.shape[0] // ALL_CROPS
        part = protos.shape[1] // dp_size
        n_proto = protos.shape[1] * vp_size
        n_rows = GLOBAL_CROPS * n_img * dp_size
        n_student = ALL_CROPS * n_img * dp_size
        depth = w_out.shape[1]
        core = lax.axis_index('core')
        data_idx = (lax.axis_index('y') * 2 + lax.axis_index('x')) * 2 + core
        protos_own = lax.dynamic_slice_in_dim(protos, data_idx * part, part, axis=1)
        ema_own = lax.dynamic_slice_in_dim(ema_protos, data_idx * part, part, axis=1)

        own_x = view_major(student_x, n_img, ALL_CROPS)
        own_tx = view_major(teacher_x, n_img, GLOBAL_CROPS)
        t_proj = mlp_project(own_tx, ema_w_in, ema_b_in, ema_w_mid, ema_b_mid, ema_w_out, ema_b_out)
        s_proj = mlp_project(own_x, w_in, b_in, w_mid, b_mid, w_out, b_out)
        both = gather_rows(jnp.concatenate([t_proj, s_proj], axis=0)[None], data)
        both, own_x = lax.optimization_barrier((both, own_x))
        t_all = unit_rows(both[:, :t_proj.shape[0]].reshape(n_rows, depth))
        s_all = unit_rows(both[:, t_proj.shape[0]:].reshape(n_student, depth))
        half_x = round_rows(gather_rows(own_x, ('y', 'x')))

        q_hi, q_lo, q_row = sinkhorn(t_all, ema_own, sizes, n_proto)
        exp_lo, row_part, exp_u, hi_u, lo_u = soft_pass(s_all, protos_own, q_hi, q_lo)
        row_sum = total_rows(row_part, sizes)

        scale = 1.0 / (n_img * dp_size * GLOBAL_CROPS * (ALL_CROPS - 1))
        counts = jnp.broadcast_to(crop_counts()[None, :, None], (dp_size, ALL_CROPS, n_img)).reshape(n_student)
        row_line = row_sum.reshape(-1)[:n_student]
        weight = counts / row_line
        s_views = s_all.astype(jnp.float32).reshape(dp_size, ALL_CROPS, n_img, depth)
        s_pair = (jnp.sum(s_views, axis=1, keepdims=True) - s_views[:, :GLOBAL_CROPS]).reshape(n_rows, depth)
        s_soft = s_all.astype(jnp.float32) * weight[:, None]
        g_own = grad_pass(s_soft.T.astype(jnp.bfloat16), s_pair.T.astype(jnp.bfloat16), exp_lo, q_hi, protos_own,
                          scale / TEMP_STUDENT)

        def targets_of(per_teacher):
            width = per_teacher.shape[-1]
            per_view = per_teacher.reshape(dp_size, GLOBAL_CROPS, n_img, width)
            pad = jnp.pad(per_view, ((0, 0), (0, ALL_CROPS - GLOBAL_CROPS), (0, 0), (0, 0)))
            return (jnp.sum(per_view, axis=1, keepdims=True) - pad).reshape(n_student, width)

        g_part = (weight[:, None] * exp_u - targets_of(hi_u)) * (scale / TEMP_STUDENT)
        hit_part = jnp.sum(s_pair * (hi_u + lo_u))
        packed = jnp.concatenate([g_part, jnp.broadcast_to(hit_part, (8, depth))], axis=0)
        packed, half_x = lax.optimization_barrier((packed, half_x))
        packed = lax.psum(packed, AXES)
        t_row = targets_of(q_row[:n_rows // LANES].reshape(n_rows, 1)).reshape(n_student)
        loss = (jnp.sum(t_row * jnp.log(row_line)) - packed[n_student, 0] / TEMP_STUDENT) * scale
        packed, g_own = lax.optimization_barrier((packed, g_own))
        g_protos = lax.all_gather(g_own, data, axis=1, tiled=True)

        per_dev = n_student // dp_size
        g_emb = packed[:n_student].reshape(dp_size // 2, 2, per_dev, depth)
        g_emb = lax.dynamic_slice_in_dim(g_emb, core, 1, axis=1).reshape(n_student // 2, depth)
        _, saved = mlp_forward(half_x, w_in, b_in, w_mid, b_mid, w_out, b_out)
        grads = mlp_backward(g_emb, half_x, saved, w_mid, w_out)
        swap = lambda g: g + lax.ppermute(g, 'core', [(0, 1), (1, 0)])
        biases = swap(jnp.concatenate([grads[1], grads[3], grads[5]]))
        b_grads = jnp.split(biases, [b_in.shape[0], b_in.shape[0] + b_mid.shape[0]])
        return (loss, swap(grads[0]), b_grads[0], swap(grads[2]), b_grads[1], swap(grads[4]), b_grads[2], g_protos)

    by_rows = P(data, None)
    by_cols = P(None, 'vp')
    replicated = P()
    head_specs = (replicated,) * 6
    in_specs = (by_rows, by_rows) + head_specs + (by_cols,) + head_specs + (by_cols,)
    out_specs = (replicated,) * 7 + (by_cols,)
    return jax.shard_map(local_step, mesh=fine, in_specs=in_specs, out_specs=out_specs, check_vma=False)
```

```python
import functools

import jax
import jax.numpy as jnp
from jax import lax
from jax.experimental import pallas as pl
from jax.experimental.pallas import tpu as pltpu
from jax.sharding import Mesh, PartitionSpec as P

ALL_CROPS = 10
GLOBAL_CROPS = 2
SINK_ITERS = 3
TEMP_STUDENT = 0.1
TEMP_TEACHER = 0.04


def gelu_slope(pre):
    cdf = 0.5 * (1.0 + lax.erf(pre * 0.7071067811865476))
    return cdf + pre * jnp.exp(-0.5 * pre * pre) * 0.3989422804014327


def mlp_forward(feats, w_in, b_in, w_mid, b_mid, w_out, b_out):
    pre_one = jnp.dot(feats, w_in, preferred_element_type=jnp.float32) + b_in.astype(jnp.float32)
    hid_one = jax.nn.gelu(pre_one, approximate=False).astype(jnp.bfloat16)
    pre_two = jnp.dot(hid_one, w_mid, preferred_element_type=jnp.float32) + b_mid.astype(jnp.float32)
    hid_two = jax.nn.gelu(pre_two, approximate=False).astype(jnp.bfloat16)
    proj = jnp.dot(hid_two, w_out, preferred_element_type=jnp.float32) + b_out.astype(jnp.float32)
    inv_norm = lax.rsqrt(jnp.sum(proj * proj, axis=-1, keepdims=True))
    unit = proj * inv_norm
    return unit.astype(jnp.bfloat16), (pre_one, hid_one, pre_two, hid_two, unit, inv_norm)


def mlp_backward(g_emb, feats, saved, w_mid, w_out):
    pre_one, hid_one, pre_two, hid_two, unit, inv_norm = saved
    g_proj = (g_emb - unit * jnp.sum(unit * g_emb, axis=-1, keepdims=True)) * inv_norm
    g_proj_lo = g_proj.astype(jnp.bfloat16)
    g_w_out = jnp.einsum('nh,nb->hb', hid_two, g_proj_lo, preferred_element_type=jnp.float32)
    g_hid_two = jnp.einsum('nb,hb->nh', g_proj_lo, w_out, preferred_element_type=jnp.float32)
    g_pre_two = g_hid_two.astype(jnp.bfloat16).astype(jnp.float32) * gelu_slope(pre_two)
    g_pre_two_lo = g_pre_two.astype(jnp.bfloat16)
    g_w_mid = jnp.einsum('ng,nh->gh', hid_one, g_pre_two_lo, preferred_element_type=jnp.float32)
    g_hid_one = jnp.einsum('nh,gh->ng', g_pre_two_lo, w_mid, preferred_element_type=jnp.float32)
    g_pre_one = g_hid_one.astype(jnp.bfloat16).astype(jnp.float32) * gelu_slope(pre_one)
    g_w_in = jnp.einsum('nf,nh->fh', feats, g_pre_one.astype(jnp.bfloat16), preferred_element_type=jnp.float32)
    return (g_w_in, jnp.sum(g_pre_one, axis=0), g_w_mid, jnp.sum(g_pre_two, axis=0), g_w_out, jnp.sum(g_proj, axis=0))


def col_normalize(protos):
    proto_f = protos.astype(jnp.float32)
    inv_col = lax.rsqrt(jnp.sum(proto_f * proto_f, axis=0, keepdims=True))
    unit = proto_f * inv_col
    return unit.astype(jnp.bfloat16), unit, inv_col


def col_normalize_backward(g_unit, unit, inv_col):
    return (g_unit - unit * jnp.sum(unit * g_unit, axis=0, keepdims=True)) * inv_col


def gather_rows(vals, axis_name):
    return lax.all_gather(vals.astype(jnp.float32), axis_name, axis=0, tiled=True)


def round_kernel(wide_ref, out_ref):
    out_ref[...] = wide_ref[...].astype(out_ref.dtype)


def round_rows(wide):
    rows, width = wide.shape
    block = pl.BlockSpec((rows // 4, width), lambda i: (i, 0))
    return pl.pallas_call(
        round_kernel, out_shape=jax.ShapeDtypeStruct((rows, width), jnp.bfloat16), grid=(4,),
        in_specs=[block], out_specs=block,
        cost_estimate=pl.CostEstimate(flops=rows * width, bytes_accessed=6 * rows * width, transcendentals=0))(wide)


def view_major(rows, n_img, views):
    width = rows.shape[1]
    return rows.reshape(n_img, views, width).transpose(1, 0, 2).reshape(n_img * views, width)


LANES = 128
AXES = ('vp', 'y', 'x', 'core')


def my_place(sizes):
    flat = 0
    for name, size in zip(AXES, sizes):
        flat = flat * size + lax.axis_index(name)
    return flat


def place_of(flat, sizes):
    coords = []
    for size in reversed(sizes):
        coords.append(lax.rem(flat, size))
        flat = flat // size
    return tuple(reversed(coords))


def greet_all(sizes, n_dev):
    barrier = pltpu.get_barrier_semaphore()
    me = my_place(sizes)
    for step in range(1, n_dev):
        peer = lax.rem(me + step, n_dev)
        pl.semaphore_signal(barrier, inc=1, device_id=place_of(peer, sizes), device_id_type=pl.DeviceIdType.MESH)


def await_all(n_dev):
    pl.semaphore_wait(pltpu.get_barrier_semaphore(), n_dev - 1)


def exchange(send_ref, recv_ref, send_sem, recv_sem, sizes, n_dev):
    me = my_place(sizes)
    copies = []
    for step in range(1, n_dev):
        peer = lax.rem(me + step, n_dev)
        copy = pltpu.make_async_remote_copy(
            src_ref=send_ref, dst_ref=recv_ref.at[step], send_sem=send_sem.at[step], recv_sem=recv_sem.at[step],
            device_id=place_of(peer, sizes), device_id_type=pl.DeviceIdType.MESH)
        copy.start()
        copies.append(copy)
    for copy in copies:
        copy.wait()
    total = send_ref[...]
    for step in range(1, n_dev):
        total = total + recv_ref[step]
    return total


def eye_mask():
    rows = lax.broadcasted_iota(jnp.int32, (LANES, LANES), 0)
    cols = lax.broadcasted_iota(jnp.int32, (LANES, LANES), 1)
    return rows == cols


def to_lanes(column):
    return jnp.sum(jnp.where(eye_mask(), jnp.broadcast_to(column, (LANES, LANES)), 0.0), axis=0, keepdims=True)


def to_rows(line):
    return jnp.sum(jnp.where(eye_mask(), jnp.broadcast_to(line, (LANES, LANES)), 0.0), axis=1, keepdims=True)


def fold_lanes(tile):
    total = tile[:, :LANES]
    for start in range(LANES, tile.shape[1], LANES):
        total = total + tile[:, start:start + LANES]
    return total


def head_kernel(chunk, tx_ref, sx_ref, bias_ref, *refs):
    weights, (out_ref,), bufs, (hid_one, hid_two, sems) = refs[:6], refs[6:7], refs[7:13], refs[13:]
    t_rows = tx_ref.shape[0]
    order = (0, 3, 1, 4, 2, 5)
    slot = {}
    used = 0
    for which in order:
        slot[which] = used
        span = min(chunk, weights[which].shape[1])
        for step in range(weights[which].shape[1] // span):
            cols = pl.ds(step * span, span)
            pltpu.make_async_copy(weights[which].at[:, cols], bufs[which].at[:, cols], sems.at[used]).start()
            used += 1

    def layer(which, feats, bias_row, store):
        buf = bufs[which]
        span = min(chunk, buf.shape[1])

        def one(step, carry):
            cols = pl.ds(pl.multiple_of(step * span, span), span)
            pltpu.make_async_copy(weights[which].at[:, cols], buf.at[:, cols], sems.at[slot[which] + step]).wait()
            store(cols, jnp.dot(feats[...], buf[:, cols], preferred_element_type=jnp.float32) + bias_ref[bias_row, cols])
            return carry

        lax.fori_loop(0, buf.shape[1] // span, one, 0)

    def hidden(ref, rows):
        def store(cols, pre):
            ref[rows, cols] = (0.5 * pre * (1.0 + lax.erf(pre * 0.7071067811865476))).astype(ref.dtype)
        return store

    def project(rows):
        def store(cols, proj):
            out_ref[rows, cols] = proj
        return store

    ours, theirs = pl.ds(t_rows, sx_ref.shape[0]), pl.ds(0, t_rows)
    layer(0, tx_ref, slice(0, 1), hidden(hid_one, theirs))
    layer(3, sx_ref, slice(3, 4), hidden(hid_one, ours))
    layer(1, hid_one.at[theirs], slice(1, 2), hidden(hid_two, theirs))
    layer(4, hid_one.at[ours], slice(4, 5), hidden(hid_two, ours))
    layer(2, hid_two.at[theirs], slice(2, 3), project(theirs))
    layer(5, hid_two.at[ours], slice(5, 6), project(ours))


def head_pass(own_tx, own_x, teacher, student):
    hidden = student[0].shape[1]
    lines = [jnp.pad(b.astype(jnp.float32), (0, hidden - b.shape[0])) for b in
             (teacher[1], teacher[3], teacher[5], student[1], student[3], student[5])]
    biases = jnp.stack(lines + lines[:2])
    weights = (teacher[0], teacher[2], teacher[4], student[0], student[2], student[4])
    rows = own_tx.shape[0] + own_x.shape[0]
    vmem, hbm = pl.BlockSpec(memory_space=pltpu.VMEM), pl.BlockSpec(memory_space=pl.ANY)
    return pl.pallas_call(
        functools.partial(head_kernel, 512),
        out_shape=jax.ShapeDtypeStruct((rows, student[4].shape[1]), jnp.float32),
        in_specs=[vmem] * 3 + [hbm] * 6, out_specs=vmem,
        scratch_shapes=[pltpu.VMEM(w.shape, w.dtype) for w in weights]
        + [pltpu.VMEM((rows, hidden), jnp.bfloat16)] * 2 + [pltpu.SemaphoreType.DMA((24,))],
        compiler_params=pltpu.CompilerParams(vmem_limit_bytes=56 << 20),
        cost_estimate=pl.CostEstimate(flops=10 ** 10, bytes_accessed=34 << 20, transcendentals=rows * hidden * 2),
    )(own_tx, own_x, biases, *weights)


def normal_rows(proj):
    return (proj * lax.rsqrt(jnp.sum(proj * proj, axis=-1, keepdims=True))).astype(jnp.bfloat16)


def sink_kernel(sizes, n_proto, block, both_ref, ema_ref, hi_ref, lo_ref, row_ref, s_ref,
                t_ref, v_ref, exp_ref, col_ref, scale_ref, part_ref, send_ref, recv_ref, v_sem, send_sem, recv_sem):
    n_dev = 1
    for size in sizes:
        n_dev *= size
    n_rows, width = exp_ref.shape
    groups = n_rows // LANES
    steps = width // block
    shards, per_dev, _ = both_ref.shape
    t_rows = n_rows // shards
    s_rows = per_dev - t_rows
    greet_all(sizes, n_dev)
    first = pl.multiple_of(lax.rem(my_place(sizes), shards) * width, width)
    fetch = pltpu.make_async_copy(ema_ref.at[:, pl.ds(first, width)], v_ref, v_sem)
    fetch.start()
    for shard in range(shards):
        t_ref[pl.ds(shard * t_rows, t_rows), :] = normal_rows(both_ref[shard, :t_rows, :])
        s_ref[pl.ds(shard * s_rows, s_rows), :] = normal_rows(both_ref[shard, t_rows:, :])
    fetch.wait()

    def fill(step, total):
        cols = pl.ds(pl.multiple_of(step * block, block), block)
        proto_f = v_ref[:, cols].astype(jnp.float32)
        unit = (proto_f * lax.rsqrt(jnp.sum(proto_f * proto_f, axis=0, keepdims=True))).astype(jnp.bfloat16)
        grown = jnp.exp(jnp.dot(t_ref[...], unit, preferred_element_type=jnp.float32) * (1.0 / TEMP_TEACHER))
        exp_ref[:, cols] = grown
        sums = jnp.sum(grown, axis=0, keepdims=True)
        return total + fold_lanes(sums)

    total = lax.fori_loop(0, steps, fill, jnp.zeros((1, LANES), jnp.float32))
    total = jnp.broadcast_to(jnp.sum(total, axis=1, keepdims=True), (1, LANES))
    scale_ref[...] = jnp.ones_like(scale_ref)
    await_all(n_dev)
    for it in range(SINK_ITERS):
        part_ref[...] = jnp.zeros_like(part_ref)
        lax.fori_loop(0, width // LANES, lambda s, c: sweep_at(s, c, exp_ref, scale_ref, col_ref, part_ref, n_proto), 0)
        send_ref[it] = jnp.zeros((8, LANES), jnp.float32)
        for group in range(groups):
            rows = pl.ds(group * LANES, LANES)
            send_ref[it, group:group + 1, :] = to_lanes(jnp.sum(part_ref[rows, :], axis=1, keepdims=True))
        send_ref[it, groups:groups + 1, :] = total
        sums = exchange(send_ref.at[it], recv_ref.at[it], send_sem.at[it], recv_sem.at[it], sizes, n_dev)
        crop = sums[:groups]
        if it == 0:
            whole = sums[groups:groups + 1]
            crop = crop * (whole * (1.0 / whole))
        scale = 1.0 / (crop * n_rows)
        for group in range(groups):
            rows = pl.ds(group * LANES, LANES)
            scale_ref[rows, :] = jnp.broadcast_to(to_rows(scale[group:group + 1]), (LANES, LANES))
        if it == SINK_ITERS - 1:
            row_ref[...] = jnp.zeros_like(row_ref)
            row_ref[:groups, :] = crop * scale * n_rows

    def finish(step, carry):
        cols = pl.ds(pl.multiple_of(step * LANES, LANES), LANES)
        target = exp_ref[:, cols] * scale_ref[...] * col_ref[:, cols] * n_rows
        high = target.astype(jnp.bfloat16)
        hi_ref[:, cols] = high
        lo_ref[:, cols] = (target - high.astype(jnp.float32)).astype(jnp.bfloat16)
        return carry

    lax.fori_loop(0, width // LANES, finish, 0)


def sweep_at(step, carry, exp_ref, scale_ref, col_ref, part_ref, n_proto):
    cols = pl.ds(pl.multiple_of(step * LANES, LANES), LANES)
    grown = exp_ref[:, cols]
    col = 1.0 / (jnp.sum(grown * scale_ref[...], axis=0, keepdims=True) * n_proto)
    col_ref[:, cols] = col
    part_ref[...] += grown * col
    return carry


def sinkhorn(both, ema_protos, sizes, n_proto, n_rows, width):
    shards, per_dev, depth = both.shape
    n_student = shards * per_dev - n_rows
    n_dev = 1
    for size in sizes:
        n_dev *= size
    vmem, hbm = pl.BlockSpec(memory_space=pltpu.VMEM), pl.BlockSpec(memory_space=pl.ANY)
    target = jax.ShapeDtypeStruct((n_rows, width), jnp.bfloat16)
    return pl.pallas_call(
        functools.partial(sink_kernel, sizes, n_proto, 512),
        out_shape=(target, target, jax.ShapeDtypeStruct((8, LANES), jnp.float32),
                   jax.ShapeDtypeStruct((n_student, depth), jnp.bfloat16)),
        in_specs=[vmem, hbm], out_specs=(vmem,) * 4,
        scratch_shapes=[
            pltpu.VMEM((n_rows, depth), jnp.bfloat16), pltpu.VMEM((depth, width), jnp.bfloat16),
            pltpu.VMEM((n_rows, width), jnp.float32), pltpu.VMEM((1, width), jnp.float32),
            pltpu.VMEM((n_rows, LANES), jnp.float32), pltpu.VMEM((n_rows, LANES), jnp.float32),
            pltpu.VMEM((SINK_ITERS, 8, LANES), jnp.float32), pltpu.VMEM((SINK_ITERS, n_dev, 8, LANES), jnp.float32),
            pltpu.SemaphoreType.DMA, pltpu.SemaphoreType.DMA((SINK_ITERS, n_dev)),
            pltpu.SemaphoreType.DMA((SINK_ITERS, n_dev))],
        compiler_params=pltpu.CompilerParams(collective_id=0, has_side_effects=True, vmem_limit_bytes=40 << 20),
        cost_estimate=pl.CostEstimate(flops=20 * 10 ** 9, bytes_accessed=12 << 20, transcendentals=n_rows * width),
    )(both, ema_protos)


def soft_kernel(rows, base_ref, s_ref, v_ref, hi_ref, lo_ref, exp_ref, part_ref, exp_u_ref, hi_u_ref, lo_u_ref):
    @pl.when(pl.program_id(0) == 0)
    def _():
        part_ref[...] = jnp.zeros_like(part_ref)
        exp_u_ref[...] = jnp.zeros_like(exp_u_ref)
        hi_u_ref[...] = jnp.zeros_like(hi_u_ref)
        lo_u_ref[...] = jnp.zeros_like(lo_u_ref)

    proto_f = v_ref[...].astype(jnp.float32)
    unit = (proto_f * lax.rsqrt(jnp.sum(proto_f * proto_f, axis=0, keepdims=True))).astype(jnp.bfloat16)
    across = (((1,), (1,)), ((), ()))
    hi_u_ref[...] += lax.dot_general(hi_ref[...], unit, across, preferred_element_type=jnp.float32)
    lo_u_ref[...] += lax.dot_general(lo_ref[...], unit, across, preferred_element_type=jnp.float32)

    def one(step, carry):
        at = pl.ds(pl.multiple_of(step * rows, rows), rows)
        logits = jnp.dot(s_ref[at, :], unit, preferred_element_type=jnp.float32) * (1.0 / TEMP_STUDENT)
        grown = jnp.exp(logits)
        part_ref[at, :] += fold_lanes(grown)
        low = grown.astype(jnp.bfloat16)
        exp_ref[at, :] = low
        exp_u_ref[at, :] += lax.dot_general(low, unit, across, preferred_element_type=jnp.float32)
        return carry

    lax.fori_loop(0, s_ref.shape[0] // rows, one, 0)


def soft_pass(base, s_all, protos, hi, lo):
    n_student, depth = s_all.shape
    n_rows, width = hi.shape
    block = 512
    whole = lambda shape: pl.BlockSpec(shape, lambda k, base_ref: (0, 0))
    cols = lambda height: pl.BlockSpec((height, block), lambda k, base_ref: (0, k))
    own = pl.BlockSpec((depth, block), lambda k, base_ref: (0, base_ref[0] * (width // block) + k))
    wide = lambda height, span: jax.ShapeDtypeStruct((height, span), jnp.float32)
    return pl.pallas_call(
        functools.partial(soft_kernel, 640),
        grid_spec=pltpu.PrefetchScalarGridSpec(
            num_scalar_prefetch=1, grid=(width // block,),
            in_specs=[whole((n_student, depth)), own, cols(n_rows), cols(n_rows)],
            out_specs=(cols(n_student), whole((n_student, LANES)), whole((n_student, depth)),
                       whole((n_rows, depth)), whole((n_rows, depth)))),
        out_shape=(jax.ShapeDtypeStruct((n_student, width), jnp.bfloat16), wide(n_student, LANES),
                   wide(n_student, depth), wide(n_rows, depth), wide(n_rows, depth)),
        compiler_params=pltpu.CompilerParams(dimension_semantics=('arbitrary',), vmem_limit_bytes=50 << 20),
        cost_estimate=pl.CostEstimate(flops=13 * 10 ** 9, bytes_accessed=35 << 20, transcendentals=n_student * width),
    )(base, s_all, protos, hi, lo)


def crop_weights(lines, per_dev, n_img):
    spot = (lax.broadcasted_iota(jnp.int32, (lines, LANES), 0) * LANES
            + lax.broadcasted_iota(jnp.int32, (lines, LANES), 1))
    is_global = lax.rem(spot, per_dev) < GLOBAL_CROPS * n_img
    return jnp.where(is_global, float(GLOBAL_CROPS - 1), float(GLOBAL_CROPS))


def emb_kernel(sizes, n_img, factor, part_ref, s_ref, exp_u_ref, hi_u_ref, lo_u_ref, out_ref, sum_ref, weight_ref,
               line_ref, line_recv, wide_ref, g_ref, near_recv, acc_ref, piece_recv, piece_ref, gathered,
               line_send_sem, line_recv_sem, near_send_sem, near_recv_sem,
               piece_send_sem, piece_recv_sem, all_send_sem, all_recv_sem):
    n_dev = 1
    for size in sizes:
        n_dev *= size
    chips = n_dev // 2
    shards = n_dev // sizes[0]
    n_student, depth = exp_u_ref.shape
    per_dev = n_student // shards
    groups = n_student // LANES
    mesh_type = pl.DeviceIdType.MESH
    me = my_place(sizes)
    core = lax.rem(me, 2)
    chip = me // 2
    greet_all(sizes, n_dev)
    line_ref[...] = jnp.zeros_like(line_ref)
    for group in range(groups):
        rows = pl.ds(group * LANES, LANES)
        line_ref[group:group + 1, :] = to_lanes(jnp.sum(part_ref[rows, :], axis=1, keepdims=True))

    def view_sum(shard, hits):
        base = pl.multiple_of(shard * per_dev, n_img)
        views = [s_ref[pl.ds(base + view * n_img, n_img), :].astype(jnp.float32) for view in range(ALL_CROPS)]
        total = views[0]
        for view in views[1:]:
            total = total + view
        for crop in range(GLOBAL_CROPS):
            rows = pl.ds(pl.multiple_of((shard * GLOBAL_CROPS + crop) * n_img, n_img), n_img)
            hits = hits + (total - views[crop]) * (hi_u_ref[rows, :] + lo_u_ref[rows, :])
        return hits

    hits = lax.fori_loop(0, shards, view_sum, jnp.zeros((n_img, depth), jnp.float32))
    hits = jnp.sum(jnp.sum(hits, axis=1, keepdims=True), axis=0, keepdims=True)
    line_ref[groups:groups + 1, :] = jnp.broadcast_to(hits, (1, LANES))
    await_all(n_dev)
    sums = exchange(line_ref, line_recv, line_send_sem, line_recv_sem, sizes, n_dev)
    sum_ref[...] = sums
    lines = sums.shape[0]
    weight = crop_weights(lines, per_dev, n_img) / sums
    weight_ref[...] = weight
    for group in range(groups):
        rows = pl.ds(group * LANES, LANES)
        wide_ref[rows, :] = jnp.broadcast_to(to_rows(weight[group:group + 1]), (LANES, LANES))

    def combine(shard, carry):
        to_core = lax.rem(shard, 2)
        base = pl.multiple_of(shard * per_dev, n_img)
        land = pl.multiple_of((shard // 2) * per_dev, n_img)
        tops = [hi_u_ref[pl.ds(pl.multiple_of((shard * GLOBAL_CROPS + crop) * n_img, n_img), n_img), :]
                for crop in range(GLOBAL_CROPS)]
        both = tops[0] + tops[1]
        for view in range(ALL_CROPS):
            rows = pl.ds(base + view * n_img, n_img)
            target = both - tops[view] if view < GLOBAL_CROPS else both
            wide = wide_ref[rows, :]
            soft = exp_u_ref[rows, :] * jnp.concatenate([wide, wide], axis=1)
            g_ref[to_core, pl.ds(land + view * n_img, n_img), :] = (soft - target) * factor
        return carry

    lax.fori_loop(0, shards, combine, 0)
    near = pltpu.make_async_remote_copy(
        src_ref=g_ref.at[1 - core], dst_ref=near_recv, send_sem=near_send_sem, recv_sem=near_recv_sem,
        device_id=place_of(chip * 2 + (1 - core), sizes), device_id_type=mesh_type)
    near.start()
    near.wait()
    acc_ref[...] = g_ref[core] + near_recv[...]
    piece = acc_ref.shape[0] // chips
    copies = []
    for step in range(1, chips):
        peer = lax.rem(chip + step, chips)
        copy = pltpu.make_async_remote_copy(
            src_ref=acc_ref.at[pl.ds(pl.multiple_of(peer * piece, n_img), piece)], dst_ref=piece_recv.at[step],
            send_sem=piece_send_sem.at[step], recv_sem=piece_recv_sem.at[step],
            device_id=place_of(peer * 2 + core, sizes), device_id_type=mesh_type)
        copy.start()
        copies.append(copy)
    total = acc_ref[pl.ds(pl.multiple_of(chip * piece, n_img), piece), :]
    for step in range(1, chips):
        copies[step - 1].wait()
        total = total + piece_recv[step]
    piece_ref[...] = total
    copies = []
    for step in range(1, chips):
        peer = lax.rem(chip + step, chips)
        copy = pltpu.make_async_remote_copy(
            src_ref=piece_ref, dst_ref=gathered.at[step], send_sem=all_send_sem.at[step], recv_sem=all_recv_sem.at[step],
            device_id=place_of(peer * 2 + core, sizes), device_id_type=mesh_type)
        copy.start()
        copies.append(copy)
    out_ref[pl.ds(pl.multiple_of(chip * piece, n_img), piece), :] = total
    for step in range(1, chips):
        copies[step - 1].wait()
        owner = lax.rem(chip + chips - step, chips)
        out_ref[pl.ds(pl.multiple_of(owner * piece, n_img), piece), :] = gathered[step]


def emb_grads(part, s_all, exp_u, hi_u, lo_u, sizes, n_img, factor):
    n_student, depth = exp_u.shape
    lines = (n_student // LANES // 8 + 1) * 8
    n_dev = 1
    for size in sizes:
        n_dev *= size
    half, chips = n_student // 2, n_dev // 2
    vmem = pl.BlockSpec(memory_space=pltpu.VMEM)
    wide = jnp.float32
    dma = pltpu.SemaphoreType.DMA
    return pl.pallas_call(
        functools.partial(emb_kernel, sizes, n_img, factor),
        out_shape=(jax.ShapeDtypeStruct((half, depth), wide), jax.ShapeDtypeStruct((lines, LANES), wide),
                   jax.ShapeDtypeStruct((lines, LANES), wide)),
        in_specs=[vmem] * 5, out_specs=(vmem,) * 3,
        scratch_shapes=[
            pltpu.VMEM((lines, LANES), wide), pltpu.VMEM((n_dev, lines, LANES), wide),
            pltpu.VMEM((n_student, LANES), wide), pltpu.VMEM((2, half, depth), wide), pltpu.VMEM((half, depth), wide),
            pltpu.VMEM((half, depth), wide), pltpu.VMEM((chips, half // chips, depth), wide),
            pltpu.VMEM((half // chips, depth), wide), pltpu.VMEM((chips, half // chips, depth), wide),
            dma((n_dev,)), dma((n_dev,)), dma, dma, dma((chips,)), dma((chips,)), dma((chips,)), dma((chips,))],
        compiler_params=pltpu.CompilerParams(collective_id=1, has_side_effects=True, vmem_limit_bytes=40 << 20),
        cost_estimate=pl.CostEstimate(flops=20 * 10 ** 9, bytes_accessed=8 << 20, transcendentals=0),
    )(part, s_all, exp_u, hi_u, lo_u)


def grad_kernel(factor, n_img, base_ref, weight_ref, s_ref, exp_ref, hi_ref, v_ref, out_ref, soft_ref, pair_ref):
    @pl.when(pl.program_id(0) == 0)
    def _():
        n_student = s_ref.shape[0]
        for group in range(n_student // LANES):
            rows = pl.ds(group * LANES, LANES)
            turned = s_ref[rows, :].astype(jnp.float32).T
            soft_ref[:, rows] = (turned * weight_ref[group:group + 1, :]).astype(soft_ref.dtype)
        per_dev = ALL_CROPS * n_img
        pairs = []
        for shard in range(n_student // per_dev):
            views = [s_ref[pl.ds(shard * per_dev + view * n_img, n_img), :].astype(jnp.float32)
                     for view in range(ALL_CROPS)]
            total = views[0]
            for view in views[1:]:
                total = total + view
            pairs += [total - views[crop] for crop in range(GLOBAL_CROPS)]
        per_tile = LANES // n_img
        for tile in range(len(pairs) // per_tile):
            rows = jnp.concatenate(pairs[tile * per_tile:(tile + 1) * per_tile], axis=0)
            pair_ref[:, pl.ds(tile * LANES, LANES)] = rows.T.astype(pair_ref.dtype)

    g_unit = jnp.dot(soft_ref[...], exp_ref[...], preferred_element_type=jnp.float32)
    g_unit = (g_unit - jnp.dot(pair_ref[...], hi_ref[...], preferred_element_type=jnp.float32)) * factor
    proto_f = v_ref[...].astype(jnp.float32)
    inv_col = lax.rsqrt(jnp.sum(proto_f * proto_f, axis=0, keepdims=True))
    unit = proto_f * inv_col
    out_ref[...] = (g_unit - unit * jnp.sum(unit * g_unit, axis=0, keepdims=True)) * inv_col


def grad_pass(base, weight, s_all, exp_lo, hi, protos, factor, n_img):
    n_student, depth = s_all.shape
    n_rows, width = hi.shape
    block = 512
    whole = lambda shape: pl.BlockSpec(shape, lambda k, base_ref: (0, 0))
    cols = lambda height: pl.BlockSpec((height, block), lambda k, base_ref: (0, k))
    own = pl.BlockSpec((depth, block), lambda k, base_ref: (0, base_ref[0] * (width // block) + k))
    return pl.pallas_call(
        functools.partial(grad_kernel, factor, n_img),
        grid_spec=pltpu.PrefetchScalarGridSpec(
            num_scalar_prefetch=1, grid=(width // block,),
            in_specs=[whole(weight.shape), whole((n_student, depth)), cols(n_student), cols(n_rows), own],
            out_specs=cols(depth),
            scratch_shapes=[pltpu.VMEM((depth, n_student), jnp.bfloat16), pltpu.VMEM((depth, n_rows), jnp.bfloat16)]),
        out_shape=jax.ShapeDtypeStruct((depth, width), jnp.float32),
        compiler_params=pltpu.CompilerParams(dimension_semantics=('arbitrary',), vmem_limit_bytes=40 << 20),
        cost_estimate=pl.CostEstimate(flops=7 * 10 ** 9, bytes_accessed=33 << 20, transcendentals=0),
    )(base, weight, s_all, exp_lo, hi, protos)


def solution(mesh):
    vp_size = mesh.shape['vp']
    dp_size = mesh.shape['dp']
    sizes = (vp_size, dp_size // 4, 2, 2)
    fine = Mesh(mesh.devices.reshape(sizes), AXES)
    data = ('y', 'x', 'core')

    def local_step(student_x, teacher_x, w_in, b_in, w_mid, b_mid, w_out, b_out, protos,
                   ema_w_in, ema_b_in, ema_w_mid, ema_b_mid, ema_w_out, ema_b_out, ema_protos):
        n_img = student_x.shape[0] // ALL_CROPS
        part = protos.shape[1] // dp_size
        n_proto = protos.shape[1] * vp_size
        n_rows = GLOBAL_CROPS * n_img * dp_size
        n_student = ALL_CROPS * n_img * dp_size
        core = lax.axis_index('core')
        data_idx = (lax.axis_index('y') * 2 + lax.axis_index('x')) * 2 + core
        base = data_idx.reshape(1)

        own_x = view_major(student_x, n_img, ALL_CROPS)
        own_tx = view_major(teacher_x, n_img, GLOBAL_CROPS)
        both = head_pass(own_tx, own_x, (ema_w_in, ema_b_in, ema_w_mid, ema_b_mid, ema_w_out, ema_b_out),
                         (w_in, b_in, w_mid, b_mid, w_out, b_out))
        both = gather_rows(both[None], data)
        both, own_x = lax.optimization_barrier((both, own_x))
        half_wide = gather_rows(own_x, ('y', 'x'))

        q_hi, q_lo, q_row, s_all = sinkhorn(both, ema_protos, sizes, n_proto, n_rows, part)
        exp_lo, row_part, exp_u, hi_u, lo_u = soft_pass(base, s_all, protos, q_hi, q_lo)
        scale = 1.0 / (n_img * dp_size * GLOBAL_CROPS * (ALL_CROPS - 1))
        factor = scale / TEMP_STUDENT
        g_emb, sums, weight = emb_grads(row_part, s_all, exp_u, hi_u, lo_u, sizes, n_img, factor)
        g_own = grad_pass(base, weight, s_all, exp_lo, q_hi, protos, factor, n_img)
        g_own, half_wide = lax.optimization_barrier((g_own, half_wide))
        g_protos = lax.all_gather(g_own, data, axis=1, tiled=True)
        half_x = round_rows(half_wide)

        per_view = q_row[:n_rows // LANES].reshape(dp_size, GLOBAL_CROPS, n_img)
        pad = jnp.pad(per_view, ((0, 0), (0, ALL_CROPS - GLOBAL_CROPS), (0, 0)))
        t_row = (jnp.sum(per_view, axis=1, keepdims=True) - pad).reshape(-1)
        row_line = sums.reshape(-1)[:n_student]
        hits = sums[n_student // LANES, 0]
        loss = (jnp.sum(t_row * jnp.log(row_line)) - hits / TEMP_STUDENT) * scale

        _, saved = mlp_forward(half_x, w_in, b_in, w_mid, b_mid, w_out, b_out)
        grads = mlp_backward(g_emb, half_x, saved, w_mid, w_out)
        swap = lambda g: g + lax.ppermute(g, 'core', [(0, 1), (1, 0)])
        biases = swap(jnp.concatenate([grads[1], grads[3], grads[5]]))
        b_grads = jnp.split(biases, [b_in.shape[0], b_in.shape[0] + b_mid.shape[0]])
        return (loss, swap(grads[0]), b_grads[0], swap(grads[2]), b_grads[1], swap(grads[4]), b_grads[2], g_protos)

    by_rows = P(data, None)
    by_cols = P(None, 'vp')
    replicated = P()
    head_specs = (replicated,) * 6
    in_specs = (by_rows, by_rows) + head_specs + (by_cols,) + head_specs + (by_cols,)
    out_specs = (replicated,) * 7 + (by_cols,)
    return jax.shard_map(local_step, mesh=fine, in_specs=in_specs, out_specs=out_specs, check_vma=False)
```

```python
import functools

import jax
import jax.numpy as jnp
from jax import lax
from jax.experimental import pallas as pl
from jax.experimental.pallas import tpu as pltpu
from jax.sharding import Mesh, PartitionSpec as P

ALL_CROPS = 10
GLOBAL_CROPS = 2
SINK_ITERS = 3
TEMP_STUDENT = 0.1
TEMP_TEACHER = 0.04


def layer_kernel(rows, feats_ref, w_ref, bias_ref, hid_ref, slope_ref, *narrow):
    if narrow:
        @pl.when(pl.program_id(0) == 0)
        def _():
            narrow[0][...] = feats_ref[...].astype(jnp.bfloat16)
        feats_ref = narrow[0]

    def one(step, carry):
        at = pl.ds(pl.multiple_of(step * rows, rows), rows)
        pre = jnp.dot(feats_ref[at, :], w_ref[...], preferred_element_type=jnp.float32) + bias_ref[...]
        cdf = 0.5 * (1.0 + lax.erf(pre * 0.7071067811865476))
        hid_ref[at, :] = (pre * cdf).astype(hid_ref.dtype)
        slope_ref[at, :] = cdf + pre * jnp.exp(-0.5 * pre * pre) * 0.3989422804014327
        return carry

    lax.fori_loop(0, feats_ref.shape[0] // rows, one, 0)


def mlp_layer(feats, w, biases, offset):
    count, fan_in = feats.shape
    width = w.shape[1]
    block = 512
    whole = pl.BlockSpec((count, fan_in), lambda k: (0, 0))
    out = pl.BlockSpec((count, block), lambda k: (0, k))
    narrow = feats.dtype != jnp.bfloat16
    shapes = [jax.ShapeDtypeStruct((count, width), jnp.bfloat16), jax.ShapeDtypeStruct((count, width), jnp.float32)]
    return pl.pallas_call(
        functools.partial(layer_kernel, count // 4), grid=(width // block,),
        out_shape=tuple(shapes + [jax.ShapeDtypeStruct((count, fan_in), jnp.bfloat16)] * narrow),
        in_specs=[whole, pl.BlockSpec((fan_in, block), lambda k: (0, k)),
                  pl.BlockSpec((1, block), lambda k: (0, offset // block + k))],
        out_specs=tuple([out, out] + [whole] * narrow),
        compiler_params=pltpu.CompilerParams(dimension_semantics=('arbitrary',), vmem_limit_bytes=56 << 20),
        cost_estimate=pl.CostEstimate(flops=2 * count * fan_in * width, bytes_accessed=30 << 20,
                                      transcendentals=2 * count * width))(feats, w, biases)


def mlp_backward(g_emb, feats, saved, w_mid, w_out, b_out):
    hid_one, slope_one, hid_two, slope_two = saved
    proj = jnp.dot(hid_two, w_out, preferred_element_type=jnp.float32) + b_out.astype(jnp.float32)
    inv_norm = lax.rsqrt(jnp.sum(proj * proj, axis=-1, keepdims=True))
    unit = proj * inv_norm
    g_proj = (g_emb - unit * jnp.sum(unit * g_emb, axis=-1, keepdims=True)) * inv_norm
    g_proj_lo = g_proj.astype(jnp.bfloat16)
    g_w_out = jnp.einsum('nh,nb->hb', hid_two, g_proj_lo, preferred_element_type=jnp.float32)
    g_hid_two = jnp.einsum('nb,hb->nh', g_proj_lo, w_out, preferred_element_type=jnp.float32)
    g_pre_two = g_hid_two.astype(jnp.bfloat16).astype(jnp.float32) * slope_two
    g_pre_two_lo = g_pre_two.astype(jnp.bfloat16)
    g_w_mid = jnp.einsum('ng,nh->gh', hid_one, g_pre_two_lo, preferred_element_type=jnp.float32)
    g_hid_one = jnp.einsum('nh,gh->ng', g_pre_two_lo, w_mid, preferred_element_type=jnp.float32)
    g_pre_one = g_hid_one.astype(jnp.bfloat16).astype(jnp.float32) * slope_one
    g_w_in = jnp.einsum('nf,nh->fh', feats, g_pre_one.astype(jnp.bfloat16), preferred_element_type=jnp.float32)
    return (g_w_in, jnp.sum(g_pre_one, axis=0), g_w_mid, jnp.sum(g_pre_two, axis=0), g_w_out, jnp.sum(g_proj, axis=0))


def col_normalize(protos):
    proto_f = protos.astype(jnp.float32)
    inv_col = lax.rsqrt(jnp.sum(proto_f * proto_f, axis=0, keepdims=True))
    unit = proto_f * inv_col
    return unit.astype(jnp.bfloat16), unit, inv_col


def col_normalize_backward(g_unit, unit, inv_col):
    return (g_unit - unit * jnp.sum(unit * g_unit, axis=0, keepdims=True)) * inv_col


def gather_rows(vals, axis_name):
    return lax.all_gather(vals.astype(jnp.float32), axis_name, axis=0, tiled=True)


LANES = 128
AXES = ('vp', 'y', 'x', 'core')


def my_place(sizes):
    flat = 0
    for name, size in zip(AXES, sizes):
        flat = flat * size + lax.axis_index(name)
    return flat


def place_of(flat, sizes):
    coords = []
    for size in reversed(sizes):
        coords.append(lax.rem(flat, size))
        flat = flat // size
    return tuple(reversed(coords))


def greet_all(sizes, n_dev):
    barrier = pltpu.get_barrier_semaphore()
    me = my_place(sizes)
    for step in range(1, n_dev):
        peer = lax.rem(me + step, n_dev)
        pl.semaphore_signal(barrier, inc=1, device_id=place_of(peer, sizes), device_id_type=pl.DeviceIdType.MESH)


def await_all(n_dev):
    pl.semaphore_wait(pltpu.get_barrier_semaphore(), n_dev - 1)


def exchange(send_ref, recv_ref, send_sem, recv_sem, sizes, n_dev):
    me = my_place(sizes)
    copies = []
    for step in range(1, n_dev):
        peer = lax.rem(me + step, n_dev)
        copy = pltpu.make_async_remote_copy(
            src_ref=send_ref, dst_ref=recv_ref.at[step], send_sem=send_sem.at[step], recv_sem=recv_sem.at[step],
            device_id=place_of(peer, sizes), device_id_type=pl.DeviceIdType.MESH)
        copy.start()
        copies.append(copy)
    for copy in copies:
        copy.wait()
    total = send_ref[...]
    for step in range(1, n_dev):
        total = total + recv_ref[step]
    return total


def eye_mask():
    rows = lax.broadcasted_iota(jnp.int32, (LANES, LANES), 0)
    cols = lax.broadcasted_iota(jnp.int32, (LANES, LANES), 1)
    return rows == cols


def to_lanes(column):
    return jnp.sum(jnp.where(eye_mask(), jnp.broadcast_to(column, (LANES, LANES)), 0.0), axis=0, keepdims=True)


def to_rows(line):
    return jnp.sum(jnp.where(eye_mask(), jnp.broadcast_to(line, (LANES, LANES)), 0.0), axis=1, keepdims=True)


def fold_lanes(tile):
    total = tile[:, :LANES]
    for start in range(LANES, tile.shape[1], LANES):
        total = total + tile[:, start:start + LANES]
    return total


def head_kernel(chunk, offsets, tx_ref, sx_ref, bias_ref, *refs):
    weights, (out_ref,), bufs, (hid_one, hid_two, proj_ref, sems) = refs[:6], refs[6:7], refs[7:13], refs[13:]
    t_rows = tx_ref.shape[0]
    order = (0, 3, 1, 4, 2, 5)
    slot = {}
    used = 0
    for which in order:
        slot[which] = used
        span = min(chunk, weights[which].shape[1])
        for step in range(weights[which].shape[1] // span):
            cols = pl.ds(step * span, span)
            pltpu.make_async_copy(weights[which].at[:, cols], bufs[which].at[:, cols], sems.at[used]).start()
            used += 1

    def layer(which, feats, store):
        buf = bufs[which]
        span = min(chunk, buf.shape[1])

        def one(step, carry):
            cols = pl.ds(pl.multiple_of(step * span, span), span)
            pltpu.make_async_copy(weights[which].at[:, cols], buf.at[:, cols], sems.at[slot[which] + step]).wait()
            bias_at = pl.ds(pl.multiple_of(offsets[which] + step * span, LANES), span)
            store(cols, jnp.dot(feats[...], buf[:, cols], preferred_element_type=jnp.float32) + bias_ref[:, bias_at])
            return carry

        lax.fori_loop(0, buf.shape[1] // span, one, 0)

    def hidden(ref, rows):
        def store(cols, pre):
            ref[rows, cols] = (0.5 * pre * (1.0 + lax.erf(pre * 0.7071067811865476))).astype(ref.dtype)
        return store

    def project(rows):
        def store(cols, proj):
            for lane in range(proj_ref.shape[0]):
                proj_ref[lane, rows, :] = proj[:, lane * LANES:(lane + 1) * LANES]
        return store

    ours, theirs = pl.ds(t_rows, sx_ref.shape[0]), pl.ds(0, t_rows)
    layer(0, tx_ref, hidden(hid_one, theirs))
    layer(3, sx_ref, hidden(hid_one, ours))
    layer(1, hid_one.at[theirs], hidden(hid_two, theirs))
    layer(4, hid_one.at[ours], hidden(hid_two, ours))
    layer(2, hid_two.at[theirs], project(theirs))
    layer(5, hid_two.at[ours], project(ours))
    for start, views, count in ((0, GLOBAL_CROPS, t_rows), (t_rows, ALL_CROPS, sx_ref.shape[0])):
        n_img = count // views
        for view in range(views):
            for lane in range(proj_ref.shape[0]):
                at = pl.ds(lane * LANES, LANES)
                rows = pl.ds(start + view, n_img, stride=views)
                out_ref[pl.ds(start + view * n_img, n_img), at] = proj_ref[lane, rows, :]


def head_pass(own_tx, own_x, biases, offsets, teacher, student):
    hidden = student[0].shape[1]
    weights = teacher + student
    rows = own_tx.shape[0] + own_x.shape[0]
    vmem, hbm = pl.BlockSpec(memory_space=pltpu.VMEM), pl.BlockSpec(memory_space=pl.ANY)
    return pl.pallas_call(
        functools.partial(head_kernel, 512, offsets),
        out_shape=jax.ShapeDtypeStruct((rows, student[2].shape[1]), jnp.float32),
        in_specs=[vmem] * 3 + [hbm] * 6, out_specs=vmem,
        scratch_shapes=[pltpu.VMEM(w.shape, w.dtype) for w in weights]
        + [pltpu.VMEM((rows, hidden), jnp.bfloat16)] * 2 + [pltpu.VMEM((student[2].shape[1] // LANES, rows, LANES), jnp.float32)] + [pltpu.SemaphoreType.DMA((24,))],
        compiler_params=pltpu.CompilerParams(vmem_limit_bytes=56 << 20),
        cost_estimate=pl.CostEstimate(flops=10 ** 10, bytes_accessed=34 << 20, transcendentals=rows * hidden * 2),
    )(own_tx, own_x, biases, *weights)


def normal_rows(proj):
    return (proj * lax.rsqrt(jnp.sum(proj * proj, axis=-1, keepdims=True))).astype(jnp.bfloat16)


def sink_kernel(sizes, n_proto, block, both_ref, ema_ref, hi_ref, lo_ref, row_ref, s_ref,
                t_ref, v_ref, exp_ref, col_ref, scale_ref, part_ref, send_ref, recv_ref, v_sem, send_sem, recv_sem):
    n_dev = 1
    for size in sizes:
        n_dev *= size
    n_rows, width = exp_ref.shape
    groups = n_rows // LANES
    steps = width // block
    shards, per_dev, _ = both_ref.shape
    t_rows = n_rows // shards
    s_rows = per_dev - t_rows
    greet_all(sizes, n_dev)
    first = pl.multiple_of(lax.rem(my_place(sizes), shards) * width, width)
    fetch = pltpu.make_async_copy(ema_ref.at[:, pl.ds(first, width)], v_ref, v_sem)
    fetch.start()
    for shard in range(shards):
        t_ref[pl.ds(shard * t_rows, t_rows), :] = normal_rows(both_ref[shard, :t_rows, :])
        s_ref[pl.ds(shard * s_rows, s_rows), :] = normal_rows(both_ref[shard, t_rows:, :])
    fetch.wait()

    def fill(step, total):
        cols = pl.ds(pl.multiple_of(step * block, block), block)
        proto_f = v_ref[:, cols].astype(jnp.float32)
        unit = (proto_f * lax.rsqrt(jnp.sum(proto_f * proto_f, axis=0, keepdims=True))).astype(jnp.bfloat16)
        grown = jnp.exp(jnp.dot(t_ref[...], unit, preferred_element_type=jnp.float32) * (1.0 / TEMP_TEACHER))
        exp_ref[:, cols] = grown
        sums = jnp.sum(grown, axis=0, keepdims=True)
        return total + fold_lanes(sums)

    total = lax.fori_loop(0, steps, fill, jnp.zeros((1, LANES), jnp.float32))
    total = jnp.broadcast_to(jnp.sum(total, axis=1, keepdims=True), (1, LANES))
    scale_ref[...] = jnp.ones_like(scale_ref)
    await_all(n_dev)
    for it in range(SINK_ITERS):
        part_ref[...] = jnp.zeros_like(part_ref)
        lax.fori_loop(0, width // LANES, lambda s, c: sweep_at(s, c, exp_ref, scale_ref, col_ref, part_ref, n_proto), 0)
        send_ref[it] = jnp.zeros((8, LANES), jnp.float32)
        for group in range(groups):
            rows = pl.ds(group * LANES, LANES)
            send_ref[it, group:group + 1, :] = to_lanes(jnp.sum(part_ref[rows, :], axis=1, keepdims=True))
        send_ref[it, groups:groups + 1, :] = total
        sums = exchange(send_ref.at[it], recv_ref.at[it], send_sem.at[it], recv_sem.at[it], sizes, n_dev)
        crop = sums[:groups]
        if it == 0:
            whole = sums[groups:groups + 1]
            crop = crop * (whole * (1.0 / whole))
        scale = 1.0 / (crop * n_rows)
        for group in range(groups):
            rows = pl.ds(group * LANES, LANES)
            scale_ref[rows, :] = jnp.broadcast_to(to_rows(scale[group:group + 1]), (LANES, LANES))
        if it == SINK_ITERS - 1:
            row_ref[...] = jnp.zeros_like(row_ref)
            row_ref[:groups, :] = crop * scale * n_rows

    def finish(step, carry):
        cols = pl.ds(pl.multiple_of(step * LANES, LANES), LANES)
        target = exp_ref[:, cols] * scale_ref[...] * col_ref[:, cols] * n_rows
        high = target.astype(jnp.bfloat16)
        hi_ref[:, cols] = high
        lo_ref[:, cols] = (target - high.astype(jnp.float32)).astype(jnp.bfloat16)
        return carry

    lax.fori_loop(0, width // LANES, finish, 0)


def sweep_at(step, carry, exp_ref, scale_ref, col_ref, part_ref, n_proto):
    cols = pl.ds(pl.multiple_of(step * LANES, LANES), LANES)
    grown = exp_ref[:, cols]
    col = 1.0 / (jnp.sum(grown * scale_ref[...], axis=0, keepdims=True) * n_proto)
    col_ref[:, cols] = col
    part_ref[...] += grown * col
    return carry


def sinkhorn(both, ema_protos, sizes, n_proto, n_rows, width):
    shards, per_dev, depth = both.shape
    n_student = shards * per_dev - n_rows
    n_dev = 1
    for size in sizes:
        n_dev *= size
    vmem, hbm = pl.BlockSpec(memory_space=pltpu.VMEM), pl.BlockSpec(memory_space=pl.ANY)
    target = jax.ShapeDtypeStruct((n_rows, width), jnp.bfloat16)
    return pl.pallas_call(
        functools.partial(sink_kernel, sizes, n_proto, 512),
        out_shape=(target, target, jax.ShapeDtypeStruct((8, LANES), jnp.float32),
                   jax.ShapeDtypeStruct((n_student, depth), jnp.bfloat16)),
        in_specs=[vmem, hbm], out_specs=(vmem,) * 4,
        scratch_shapes=[
            pltpu.VMEM((n_rows, depth), jnp.bfloat16), pltpu.VMEM((depth, width), jnp.bfloat16),
            pltpu.VMEM((n_rows, width), jnp.float32), pltpu.VMEM((1, width), jnp.float32),
            pltpu.VMEM((n_rows, LANES), jnp.float32), pltpu.VMEM((n_rows, LANES), jnp.float32),
            pltpu.VMEM((SINK_ITERS, 8, LANES), jnp.float32), pltpu.VMEM((SINK_ITERS, n_dev, 8, LANES), jnp.float32),
            pltpu.SemaphoreType.DMA, pltpu.SemaphoreType.DMA((SINK_ITERS, n_dev)),
            pltpu.SemaphoreType.DMA((SINK_ITERS, n_dev))],
        compiler_params=pltpu.CompilerParams(collective_id=0, has_side_effects=True, vmem_limit_bytes=40 << 20),
        cost_estimate=pl.CostEstimate(flops=20 * 10 ** 9, bytes_accessed=12 << 20, transcendentals=n_rows * width),
    )(both, ema_protos)


def soft_kernel(rows, base_ref, s_ref, v_ref, hi_ref, lo_ref, exp_ref, part_ref, exp_u_ref, hi_u_ref, lo_u_ref):
    @pl.when(pl.program_id(0) == 0)
    def _():
        part_ref[...] = jnp.zeros_like(part_ref)
        exp_u_ref[...] = jnp.zeros_like(exp_u_ref)
        hi_u_ref[...] = jnp.zeros_like(hi_u_ref)
        lo_u_ref[...] = jnp.zeros_like(lo_u_ref)

    proto_f = v_ref[...].astype(jnp.float32)
    unit = (proto_f * lax.rsqrt(jnp.sum(proto_f * proto_f, axis=0, keepdims=True))).astype(jnp.bfloat16)
    across = (((1,), (1,)), ((), ()))
    hi_u_ref[...] += lax.dot_general(hi_ref[...], unit, across, preferred_element_type=jnp.float32)
    lo_u_ref[...] += lax.dot_general(lo_ref[...], unit, across, preferred_element_type=jnp.float32)

    def one(step, carry):
        at = pl.ds(pl.multiple_of(step * rows, rows), rows)
        logits = jnp.dot(s_ref[at, :], unit, preferred_element_type=jnp.float32) * (1.0 / TEMP_STUDENT)
        grown = jnp.exp(logits)
        part_ref[at, :] += fold_lanes(grown)
        low = grown.astype(jnp.bfloat16)
        exp_ref[at, :] = low
        exp_u_ref[at, :] += lax.dot_general(low, unit, across, preferred_element_type=jnp.float32)
        return carry

    lax.fori_loop(0, s_ref.shape[0] // rows, one, 0)


def soft_pass(base, s_all, protos, hi, lo):
    n_student, depth = s_all.shape
    n_rows, width = hi.shape
    block = 512
    whole = lambda shape: pl.BlockSpec(shape, lambda k, base_ref: (0, 0))
    cols = lambda height: pl.BlockSpec((height, block), lambda k, base_ref: (0, k))
    own = pl.BlockSpec((depth, block), lambda k, base_ref: (0, base_ref[0] * (width // block) + k))
    wide = lambda height, span: jax.ShapeDtypeStruct((height, span), jnp.float32)
    return pl.pallas_call(
        functools.partial(soft_kernel, 640),
        grid_spec=pltpu.PrefetchScalarGridSpec(
            num_scalar_prefetch=1, grid=(width // block,),
            in_specs=[whole((n_student, depth)), own, cols(n_rows), cols(n_rows)],
            out_specs=(cols(n_student), whole((n_student, LANES)), whole((n_student, depth)),
                       whole((n_rows, depth)), whole((n_rows, depth)))),
        out_shape=(jax.ShapeDtypeStruct((n_student, width), jnp.bfloat16), wide(n_student, LANES),
                   wide(n_student, depth), wide(n_rows, depth), wide(n_rows, depth)),
        compiler_params=pltpu.CompilerParams(dimension_semantics=('arbitrary',), vmem_limit_bytes=50 << 20),
        cost_estimate=pl.CostEstimate(flops=13 * 10 ** 9, bytes_accessed=35 << 20, transcendentals=n_student * width),
    )(base, s_all, protos, hi, lo)


def crop_weights(lines, per_dev, n_img):
    spot = (lax.broadcasted_iota(jnp.int32, (lines, LANES), 0) * LANES
            + lax.broadcasted_iota(jnp.int32, (lines, LANES), 1))
    is_global = lax.rem(spot, per_dev) < GLOBAL_CROPS * n_img
    return jnp.where(is_global, float(GLOBAL_CROPS - 1), float(GLOBAL_CROPS))


def line_kernel(sizes, n_img, part_ref, s_ref, hi_u_ref, lo_u_ref, sum_ref, weight_ref,
                line_ref, line_recv, line_send_sem, line_recv_sem):
    n_dev = 1
    for size in sizes:
        n_dev *= size
    shards = n_dev // sizes[0]
    n_student, depth = s_ref.shape
    per_dev = n_student // shards
    groups = n_student // LANES
    greet_all(sizes, n_dev)
    line_ref[...] = jnp.zeros_like(line_ref)
    for group in range(groups):
        rows = pl.ds(group * LANES, LANES)
        line_ref[group:group + 1, :] = to_lanes(jnp.sum(part_ref[rows, :], axis=1, keepdims=True))

    def view_sum(shard, hits):
        base = pl.multiple_of(shard * per_dev, n_img)
        views = [s_ref[pl.ds(base + view * n_img, n_img), :].astype(jnp.float32) for view in range(ALL_CROPS)]
        total = views[0]
        for view in views[1:]:
            total = total + view
        for crop in range(GLOBAL_CROPS):
            rows = pl.ds(pl.multiple_of((shard * GLOBAL_CROPS + crop) * n_img, n_img), n_img)
            hits = hits + (total - views[crop]) * (hi_u_ref[rows, :] + lo_u_ref[rows, :])
        return hits

    hits = lax.fori_loop(0, shards, view_sum, jnp.zeros((n_img, depth), jnp.float32))
    hits = jnp.sum(jnp.sum(hits, axis=1, keepdims=True), axis=0, keepdims=True)
    line_ref[groups:groups + 1, :] = jnp.broadcast_to(hits, (1, LANES))
    await_all(n_dev)
    sums = exchange(line_ref, line_recv, line_send_sem, line_recv_sem, sizes, n_dev)
    sum_ref[...] = sums
    lines = sums.shape[0]
    weight_ref[...] = crop_weights(lines, per_dev, n_img) / sums


def emb_kernel(sizes, n_img, factor, weight_ref, exp_u_ref, hi_u_ref, out_ref,
               wide_ref, g_ref, near_recv, acc_ref, piece_recv, piece_ref, gathered, full_ref,
               near_send_sem, near_recv_sem, piece_send_sem, piece_recv_sem, all_send_sem, all_recv_sem):
    n_dev = 1
    for size in sizes:
        n_dev *= size
    chips = n_dev // 2
    shards = n_dev // sizes[0]
    n_student, depth = exp_u_ref.shape
    per_dev = n_student // shards
    groups = n_student // LANES
    mesh_type = pl.DeviceIdType.MESH
    me = my_place(sizes)
    core = lax.rem(me, 2)
    chip = me // 2
    greet_all(sizes, n_dev)
    weight = weight_ref[...]
    for group in range(groups):
        rows = pl.ds(group * LANES, LANES)
        wide_ref[rows, :] = jnp.broadcast_to(to_rows(weight[group:group + 1]), (LANES, LANES))

    def combine(shard, carry):
        to_core = lax.rem(shard, 2)
        base = pl.multiple_of(shard * per_dev, n_img)
        land = pl.multiple_of((shard // 2) * per_dev, n_img)
        tops = [hi_u_ref[pl.ds(pl.multiple_of((shard * GLOBAL_CROPS + crop) * n_img, n_img), n_img), :]
                for crop in range(GLOBAL_CROPS)]
        both = tops[0] + tops[1]
        for view in range(ALL_CROPS):
            rows = pl.ds(base + view * n_img, n_img)
            target = both - tops[view] if view < GLOBAL_CROPS else both
            wide = wide_ref[rows, :]
            soft = exp_u_ref[rows, :] * jnp.concatenate([wide, wide], axis=1)
            g_ref[to_core, pl.ds(land + view * n_img, n_img), :] = (soft - target) * factor
        return carry

    lax.fori_loop(0, shards, combine, 0)
    await_all(n_dev)
    near = pltpu.make_async_remote_copy(
        src_ref=g_ref.at[1 - core], dst_ref=near_recv, send_sem=near_send_sem, recv_sem=near_recv_sem,
        device_id=place_of(chip * 2 + (1 - core), sizes), device_id_type=mesh_type)
    near.start()
    near.wait()
    acc_ref[...] = g_ref[core] + near_recv[...]
    piece = acc_ref.shape[0] // chips
    copies = []
    for step in range(1, chips):
        peer = lax.rem(chip + step, chips)
        copy = pltpu.make_async_remote_copy(
            src_ref=acc_ref.at[pl.ds(pl.multiple_of(peer * piece, n_img), piece)], dst_ref=piece_recv.at[step],
            send_sem=piece_send_sem.at[step], recv_sem=piece_recv_sem.at[step],
            device_id=place_of(peer * 2 + core, sizes), device_id_type=mesh_type)
        copy.start()
        copies.append(copy)
    total = acc_ref[pl.ds(pl.multiple_of(chip * piece, n_img), piece), :]
    for step in range(1, chips):
        copies[step - 1].wait()
        total = total + piece_recv[step]
    piece_ref[...] = total
    copies = []
    for step in range(1, chips):
        peer = lax.rem(chip + step, chips)
        copy = pltpu.make_async_remote_copy(
            src_ref=piece_ref, dst_ref=gathered.at[step], send_sem=all_send_sem.at[step], recv_sem=all_recv_sem.at[step],
            device_id=place_of(peer * 2 + core, sizes), device_id_type=mesh_type)
        copy.start()
        copies.append(copy)
    full_ref[pl.ds(pl.multiple_of(chip * piece, n_img), piece), :] = total
    for step in range(1, chips):
        copies[step - 1].wait()
        owner = lax.rem(chip + chips - step, chips)
        full_ref[pl.ds(pl.multiple_of(owner * piece, n_img), piece), :] = gathered[step]
    for base in range(0, full_ref.shape[0], per_dev):
        for view in range(ALL_CROPS):
            for lane in range(depth // LANES):
                at = pl.ds(lane * LANES, LANES)
                rows = pl.ds(base + view, n_img, stride=ALL_CROPS)
                out_ref[lane, rows, :] = full_ref[pl.ds(base + view * n_img, n_img), at]


def crop_lines(part, s_all, hi_u, lo_u, sizes, n_img):
    lines = (part.shape[0] // LANES // 8 + 1) * 8
    n_dev = 1
    for size in sizes:
        n_dev *= size
    vmem = pl.BlockSpec(memory_space=pltpu.VMEM)
    line = jax.ShapeDtypeStruct((lines, LANES), jnp.float32)
    return pl.pallas_call(
        functools.partial(line_kernel, sizes, n_img), out_shape=(line, line), in_specs=[vmem] * 4, out_specs=(vmem,) * 2,
        scratch_shapes=[
            pltpu.VMEM((lines, LANES), jnp.float32), pltpu.VMEM((n_dev, lines, LANES), jnp.float32),
            pltpu.SemaphoreType.DMA((n_dev,)), pltpu.SemaphoreType.DMA((n_dev,))],
        compiler_params=pltpu.CompilerParams(collective_id=1, has_side_effects=True, vmem_limit_bytes=24 << 20),
        cost_estimate=pl.CostEstimate(flops=5 * 10 ** 9, bytes_accessed=4 << 20, transcendentals=0),
    )(part, s_all, hi_u, lo_u)


def emb_grads(weight, exp_u, hi_u, sizes, n_img, factor):
    n_student, depth = exp_u.shape
    n_dev = 1
    for size in sizes:
        n_dev *= size
    half, chips = n_student // 2, n_dev // 2
    vmem = pl.BlockSpec(memory_space=pltpu.VMEM)
    wide = jnp.float32
    dma = pltpu.SemaphoreType.DMA
    return pl.pallas_call(
        functools.partial(emb_kernel, sizes, n_img, factor),
        out_shape=jax.ShapeDtypeStruct((depth // LANES, half, LANES), wide), in_specs=[vmem] * 3, out_specs=vmem,
        scratch_shapes=[
            pltpu.VMEM((n_student, LANES), wide), pltpu.VMEM((2, half, depth), wide), pltpu.VMEM((half, depth), wide),
            pltpu.VMEM((half, depth), wide), pltpu.VMEM((chips, half // chips, depth), wide),
            pltpu.VMEM((half // chips, depth), wide), pltpu.VMEM((chips, half // chips, depth), wide),
            pltpu.VMEM((half, depth), wide),
            dma, dma, dma((chips,)), dma((chips,)), dma((chips,)), dma((chips,))],
        compiler_params=pltpu.CompilerParams(collective_id=2, has_side_effects=True, vmem_limit_bytes=32 << 20),
        cost_estimate=pl.CostEstimate(flops=20 * 10 ** 9, bytes_accessed=8 << 20, transcendentals=0),
    )(weight, exp_u, hi_u)


def grad_kernel(factor, n_img, base_ref, weight_ref, s_ref, exp_ref, hi_ref, v_ref, out_ref, soft_ref, pair_ref):
    @pl.when(pl.program_id(0) == 0)
    def _():
        n_student = s_ref.shape[0]
        for group in range(n_student // LANES):
            rows = pl.ds(group * LANES, LANES)
            turned = s_ref[rows, :].astype(jnp.float32).T
            soft_ref[:, rows] = (turned * weight_ref[group:group + 1, :]).astype(soft_ref.dtype)
        per_dev = ALL_CROPS * n_img
        pairs = []
        for shard in range(n_student // per_dev):
            views = [s_ref[pl.ds(shard * per_dev + view * n_img, n_img), :].astype(jnp.float32)
                     for view in range(ALL_CROPS)]
            total = views[0]
            for view in views[1:]:
                total = total + view
            pairs += [total - views[crop] for crop in range(GLOBAL_CROPS)]
        per_tile = LANES // n_img
        for tile in range(len(pairs) // per_tile):
            rows = jnp.concatenate(pairs[tile * per_tile:(tile + 1) * per_tile], axis=0)
            pair_ref[:, pl.ds(tile * LANES, LANES)] = rows.T.astype(pair_ref.dtype)

    g_unit = jnp.dot(soft_ref[...], exp_ref[...], preferred_element_type=jnp.float32)
    g_unit = (g_unit - jnp.dot(pair_ref[...], hi_ref[...], preferred_element_type=jnp.float32)) * factor
    proto_f = v_ref[...].astype(jnp.float32)
    inv_col = lax.rsqrt(jnp.sum(proto_f * proto_f, axis=0, keepdims=True))
    unit = proto_f * inv_col
    out_ref[...] = (g_unit - unit * jnp.sum(unit * g_unit, axis=0, keepdims=True)) * inv_col


def grad_pass(base, weight, s_all, exp_lo, hi, protos, factor, n_img):
    n_student, depth = s_all.shape
    n_rows, width = hi.shape
    block = 512
    whole = lambda shape: pl.BlockSpec(shape, lambda k, base_ref: (0, 0))
    cols = lambda height: pl.BlockSpec((height, block), lambda k, base_ref: (0, k))
    own = pl.BlockSpec((depth, block), lambda k, base_ref: (0, base_ref[0] * (width // block) + k))
    return pl.pallas_call(
        functools.partial(grad_kernel, factor, n_img),
        grid_spec=pltpu.PrefetchScalarGridSpec(
            num_scalar_prefetch=1, grid=(width // block,),
            in_specs=[whole(weight.shape), whole((n_student, depth)), cols(n_student), cols(n_rows), own],
            out_specs=cols(depth),
            scratch_shapes=[pltpu.VMEM((depth, n_student), jnp.bfloat16), pltpu.VMEM((depth, n_rows), jnp.bfloat16)]),
        out_shape=jax.ShapeDtypeStruct((depth, width), jnp.float32),
        compiler_params=pltpu.CompilerParams(dimension_semantics=('arbitrary',), vmem_limit_bytes=40 << 20),
        cost_estimate=pl.CostEstimate(flops=7 * 10 ** 9, bytes_accessed=33 << 20, transcendentals=0),
    )(base, weight, s_all, exp_lo, hi, protos)


def solution(mesh):
    vp_size = mesh.shape['vp']
    dp_size = mesh.shape['dp']
    sizes = (vp_size, dp_size // 4, 2, 2)
    fine = Mesh(mesh.devices.reshape(sizes), AXES)
    data = ('y', 'x', 'core')

    def local_step(student_x, teacher_x, w_in, b_in, w_mid, b_mid, w_out, b_out, protos,
                   ema_w_in, ema_b_in, ema_w_mid, ema_b_mid, ema_w_out, ema_b_out, ema_protos):
        n_img = student_x.shape[0] // ALL_CROPS
        part = protos.shape[1] // dp_size
        n_proto = protos.shape[1] * vp_size
        n_rows = GLOBAL_CROPS * n_img * dp_size
        n_student = ALL_CROPS * n_img * dp_size
        core = lax.axis_index('core')
        data_idx = (lax.axis_index('y') * 2 + lax.axis_index('x')) * 2 + core
        base = data_idx.reshape(1)

        rows_b = (ema_b_in, ema_b_mid, b_in, b_mid, ema_b_out, b_out)
        biases = jnp.concatenate(rows_b).astype(jnp.float32)[None]
        starts = []
        for row in rows_b:
            starts.append(starts[-1] + width if starts else 0)
            width = row.shape[0]
        offsets = (starts[0], starts[1], starts[4], starts[2], starts[3], starts[5])
        both = head_pass(teacher_x, student_x, biases, offsets, (ema_w_in, ema_w_mid, ema_w_out), (w_in, w_mid, w_out))
        both = gather_rows(both[None], data)
        both, own_x = lax.optimization_barrier((both, student_x))
        half_wide = gather_rows(own_x, ('y', 'x'))

        q_hi, q_lo, q_row, s_all = sinkhorn(both, ema_protos, sizes, n_proto, n_rows, part)
        exp_lo, row_part, exp_u, hi_u, lo_u = soft_pass(base, s_all, protos, q_hi, q_lo)
        scale = 1.0 / (n_img * dp_size * GLOBAL_CROPS * (ALL_CROPS - 1))
        factor = scale / TEMP_STUDENT
        sums, weight = crop_lines(row_part, s_all, hi_u, lo_u, sizes, n_img)
        g_own = grad_pass(base, weight, s_all, exp_lo, q_hi, protos, factor, n_img)
        g_own, half_wide = lax.optimization_barrier((g_own, half_wide))
        g_protos = lax.all_gather(g_own, data, axis=1, tiled=True)
        weight, _ = lax.optimization_barrier((weight, g_own))
        g_emb = emb_grads(weight, exp_u, hi_u, sizes, n_img, factor)
        g_emb = jnp.concatenate([g_emb[lane] for lane in range(g_emb.shape[0])], axis=1)

        per_view = q_row[:n_rows // LANES].reshape(dp_size, GLOBAL_CROPS, n_img)
        pad = jnp.pad(per_view, ((0, 0), (0, ALL_CROPS - GLOBAL_CROPS), (0, 0)))
        t_row = (jnp.sum(per_view, axis=1, keepdims=True) - pad).reshape(-1)
        row_line = sums.reshape(-1)[:n_student]
        hits = sums[n_student // LANES, 0]
        loss = (jnp.sum(t_row * jnp.log(row_line)) - hits / TEMP_STUDENT) * scale

        hid_one, slope_one, half_x = mlp_layer(half_wide, w_in, biases, offsets[3])
        hid_two, slope_two = mlp_layer(hid_one, w_mid, biases, offsets[4])
        grads = mlp_backward(g_emb, half_x, (hid_one, slope_one, hid_two, slope_two), w_mid, w_out, b_out)
        swap = lambda g: g + lax.ppermute(g, 'core', [(0, 1), (1, 0)])
        biases = swap(jnp.concatenate([grads[1], grads[3], grads[5]]))
        b_grads = jnp.split(biases, [b_in.shape[0], b_in.shape[0] + b_mid.shape[0]])
        return (loss, swap(grads[0]), b_grads[0], swap(grads[2]), b_grads[1], swap(grads[4]), b_grads[2], g_protos)

    by_rows = P(data, None)
    by_cols = P(None, 'vp')
    replicated = P()
    head_specs = (replicated,) * 6
    in_specs = (by_rows, by_rows) + head_specs + (by_cols,) + head_specs + (by_cols,)
    out_specs = (replicated,) * 7 + (by_cols,)
    return jax.shard_map(local_step, mesh=fine, in_specs=in_specs, out_specs=out_specs, check_vma=False)
```

```python
import functools

import jax
import jax.numpy as jnp
from jax import lax
from jax.experimental import pallas as pl
from jax.experimental.pallas import tpu as pltpu
from jax.sharding import Mesh, PartitionSpec as P

ALL_CROPS = 10
GLOBAL_CROPS = 2
SINK_ITERS = 3
TEMP_STUDENT = 0.1
TEMP_TEACHER = 0.04


def layer_kernel(rows, feats_ref, w_ref, bias_ref, hid_ref, slope_ref, *narrow):
    if narrow:
        @pl.when(pl.program_id(0) == 0)
        def _():
            narrow[0][...] = feats_ref[...].astype(jnp.bfloat16)
        feats_ref = narrow[0]

    def one(step, carry):
        at = pl.ds(pl.multiple_of(step * rows, rows), rows)
        pre = jnp.dot(feats_ref[at, :], w_ref[...], preferred_element_type=jnp.float32) + bias_ref[...]
        cdf = 0.5 * (1.0 + lax.erf(pre * 0.7071067811865476))
        hid_ref[at, :] = (pre * cdf).astype(hid_ref.dtype)
        slope_ref[at, :] = cdf + pre * jnp.exp(-0.5 * pre * pre) * 0.3989422804014327
        return carry

    lax.fori_loop(0, feats_ref.shape[0] // rows, one, 0)


def mlp_layer(feats, w, biases, offset):
    count, fan_in = feats.shape
    width = w.shape[1]
    block = 512
    whole = pl.BlockSpec((count, fan_in), lambda k: (0, 0))
    out = pl.BlockSpec((count, block), lambda k: (0, k))
    narrow = feats.dtype != jnp.bfloat16
    shapes = [jax.ShapeDtypeStruct((count, width), jnp.bfloat16), jax.ShapeDtypeStruct((count, width), jnp.float32)]
    return pl.pallas_call(
        functools.partial(layer_kernel, count // 4), grid=(width // block,),
        out_shape=tuple(shapes + [jax.ShapeDtypeStruct((count, fan_in), jnp.bfloat16)] * narrow),
        in_specs=[whole, pl.BlockSpec((fan_in, block), lambda k: (0, k)),
                  pl.BlockSpec((1, block), lambda k: (0, offset // block + k))],
        out_specs=tuple([out, out] + [whole] * narrow),
        compiler_params=pltpu.CompilerParams(dimension_semantics=('arbitrary',), vmem_limit_bytes=56 << 20),
        cost_estimate=pl.CostEstimate(flops=2 * count * fan_in * width, bytes_accessed=30 << 20,
                                      transcendentals=2 * count * width))(feats, w, biases)


def mlp_backward(g_emb, feats, saved, w_mid, w_out, b_out):
    hid_one, slope_one, hid_two, slope_two = saved
    proj = jnp.dot(hid_two, w_out, preferred_element_type=jnp.float32) + b_out.astype(jnp.float32)
    inv_norm = lax.rsqrt(jnp.sum(proj * proj, axis=-1, keepdims=True))
    unit = proj * inv_norm
    g_proj = (g_emb - unit * jnp.sum(unit * g_emb, axis=-1, keepdims=True)) * inv_norm
    g_proj_lo = g_proj.astype(jnp.bfloat16)
    g_w_out = jnp.einsum('nh,nb->hb', hid_two, g_proj_lo, preferred_element_type=jnp.float32)
    g_hid_two = jnp.einsum('nb,hb->nh', g_proj_lo, w_out, preferred_element_type=jnp.float32)
    g_pre_two = g_hid_two.astype(jnp.bfloat16).astype(jnp.float32) * slope_two
    g_pre_two_lo = g_pre_two.astype(jnp.bfloat16)
    g_w_mid = jnp.einsum('ng,nh->gh', hid_one, g_pre_two_lo, preferred_element_type=jnp.float32)
    g_hid_one = jnp.einsum('nh,gh->ng', g_pre_two_lo, w_mid, preferred_element_type=jnp.float32)
    g_pre_one = g_hid_one.astype(jnp.bfloat16).astype(jnp.float32) * slope_one
    g_w_in = jnp.einsum('nf,nh->fh', feats, g_pre_one.astype(jnp.bfloat16), preferred_element_type=jnp.float32)
    return (g_w_in, jnp.sum(g_pre_one, axis=0), g_w_mid, jnp.sum(g_pre_two, axis=0), g_w_out, jnp.sum(g_proj, axis=0))


def col_normalize(protos):
    proto_f = protos.astype(jnp.float32)
    inv_col = lax.rsqrt(jnp.sum(proto_f * proto_f, axis=0, keepdims=True))
    unit = proto_f * inv_col
    return unit.astype(jnp.bfloat16), unit, inv_col


def col_normalize_backward(g_unit, unit, inv_col):
    return (g_unit - unit * jnp.sum(unit * g_unit, axis=0, keepdims=True)) * inv_col


def gather_rows(vals, axis_name):
    return lax.all_gather(vals.astype(jnp.float32), axis_name, axis=0, tiled=True)


LANES = 128
AXES = ('vp', 'y', 'x', 'core')


def my_place(sizes):
    flat = 0
    for name, size in zip(AXES, sizes):
        flat = flat * size + lax.axis_index(name)
    return flat


def place_of(flat, sizes):
    coords = []
    for size in reversed(sizes):
        coords.append(lax.rem(flat, size))
        flat = flat // size
    return tuple(reversed(coords))


def greet_all(sizes, n_dev):
    barrier = pltpu.get_barrier_semaphore()
    me = my_place(sizes)
    for step in range(1, n_dev):
        peer = lax.rem(me + step, n_dev)
        pl.semaphore_signal(barrier, inc=1, device_id=place_of(peer, sizes), device_id_type=pl.DeviceIdType.MESH)


def await_all(n_dev):
    pl.semaphore_wait(pltpu.get_barrier_semaphore(), n_dev - 1)


def exchange(send_ref, recv_ref, send_sem, recv_sem, sizes, n_dev):
    me = my_place(sizes)
    copies = []
    for step in range(1, n_dev):
        peer = lax.rem(me + step, n_dev)
        copy = pltpu.make_async_remote_copy(
            src_ref=send_ref, dst_ref=recv_ref.at[step], send_sem=send_sem.at[step], recv_sem=recv_sem.at[step],
            device_id=place_of(peer, sizes), device_id_type=pl.DeviceIdType.MESH)
        copy.start()
        copies.append(copy)
    for copy in copies:
        copy.wait()
    total = send_ref[...]
    for step in range(1, n_dev):
        total = total + recv_ref[step]
    return total


def eye_mask():
    rows = lax.broadcasted_iota(jnp.int32, (LANES, LANES), 0)
    cols = lax.broadcasted_iota(jnp.int32, (LANES, LANES), 1)
    return rows == cols


def to_lanes(column):
    return jnp.sum(jnp.where(eye_mask(), jnp.broadcast_to(column, (LANES, LANES)), 0.0), axis=0, keepdims=True)


def to_rows(line):
    return jnp.sum(jnp.where(eye_mask(), jnp.broadcast_to(line, (LANES, LANES)), 0.0), axis=1, keepdims=True)


def fold_lanes(tile):
    total = tile[:, :LANES]
    for start in range(LANES, tile.shape[1], LANES):
        total = total + tile[:, start:start + LANES]
    return total


def head_kernel(chunk, offsets, tx_ref, sx_ref, bias_ref, *refs):
    weights, (out_ref,), bufs, (hid_one, hid_two, proj_ref, sems) = refs[:6], refs[6:7], refs[7:13], refs[13:]
    t_rows = tx_ref.shape[0]
    order = (0, 3, 1, 4, 2, 5)
    slot = {}
    used = 0
    for which in order:
        slot[which] = used
        span = min(chunk, weights[which].shape[1])
        for step in range(weights[which].shape[1] // span):
            cols = pl.ds(step * span, span)
            pltpu.make_async_copy(weights[which].at[:, cols], bufs[which].at[:, cols], sems.at[used]).start()
            used += 1

    def layer(which, feats, store):
        buf = bufs[which]
        span = min(chunk, buf.shape[1])

        def one(step, carry):
            cols = pl.ds(pl.multiple_of(step * span, span), span)
            pltpu.make_async_copy(weights[which].at[:, cols], buf.at[:, cols], sems.at[slot[which] + step]).wait()
            bias_at = pl.ds(pl.multiple_of(offsets[which] + step * span, LANES), span)
            store(cols, jnp.dot(feats[...], buf[:, cols], preferred_element_type=jnp.float32) + bias_ref[:, bias_at])
            return carry

        lax.fori_loop(0, buf.shape[1] // span, one, 0)

    def hidden(ref, rows):
        def store(cols, pre):
            ref[rows, cols] = (0.5 * pre * (1.0 + lax.erf(pre * 0.7071067811865476))).astype(ref.dtype)
        return store

    def project(rows):
        def store(cols, proj):
            for lane in range(proj_ref.shape[0]):
                proj_ref[lane, rows, :] = proj[:, lane * LANES:(lane + 1) * LANES]
        return store

    ours, theirs = pl.ds(t_rows, sx_ref.shape[0]), pl.ds(0, t_rows)
    layer(0, tx_ref, hidden(hid_one, theirs))
    layer(3, sx_ref, hidden(hid_one, ours))
    layer(1, hid_one.at[theirs], hidden(hid_two, theirs))
    layer(4, hid_one.at[ours], hidden(hid_two, ours))
    layer(2, hid_two.at[theirs], project(theirs))
    layer(5, hid_two.at[ours], project(ours))
    for start, views, count in ((0, GLOBAL_CROPS, t_rows), (t_rows, ALL_CROPS, sx_ref.shape[0])):
        n_img = count // views
        for view in range(views):
            for lane in range(proj_ref.shape[0]):
                at = pl.ds(lane * LANES, LANES)
                rows = pl.ds(start + view, n_img, stride=views)
                out_ref[pl.ds(start + view * n_img, n_img), at] = proj_ref[lane, rows, :]


def head_pass(own_tx, own_x, biases, offsets, teacher, student):
    hidden = student[0].shape[1]
    weights = teacher + student
    rows = own_tx.shape[0] + own_x.shape[0]
    vmem, hbm = pl.BlockSpec(memory_space=pltpu.VMEM), pl.BlockSpec(memory_space=pl.ANY)
    return pl.pallas_call(
        functools.partial(head_kernel, 512, offsets),
        out_shape=jax.ShapeDtypeStruct((rows, student[2].shape[1]), jnp.float32),
        in_specs=[vmem] * 3 + [hbm] * 6, out_specs=vmem,
        scratch_shapes=[pltpu.VMEM(w.shape, w.dtype) for w in weights]
        + [pltpu.VMEM((rows, hidden), jnp.bfloat16)] * 2 + [pltpu.VMEM((student[2].shape[1] // LANES, rows, LANES), jnp.float32)] + [pltpu.SemaphoreType.DMA((24,))],
        compiler_params=pltpu.CompilerParams(vmem_limit_bytes=56 << 20),
        cost_estimate=pl.CostEstimate(flops=10 ** 10, bytes_accessed=34 << 20, transcendentals=rows * hidden * 2),
    )(own_tx, own_x, biases, *weights)


def normal_rows(proj):
    return (proj * lax.rsqrt(jnp.sum(proj * proj, axis=-1, keepdims=True))).astype(jnp.bfloat16)


def sink_kernel(sizes, n_proto, block, both_ref, ema_ref, hi_ref, lo_ref, row_ref, s_ref,
                t_ref, v_ref, exp_ref, col_ref, scale_ref, part_ref, send_ref, recv_ref, v_sem, send_sem, recv_sem):
    n_dev = 1
    for size in sizes:
        n_dev *= size
    n_rows, width = exp_ref.shape
    groups = n_rows // LANES
    steps = width // block
    shards, per_dev, _ = both_ref.shape
    t_rows = n_rows // shards
    s_rows = per_dev - t_rows
    greet_all(sizes, n_dev)
    first = pl.multiple_of(lax.rem(my_place(sizes), shards) * width, width)
    fetch = pltpu.make_async_copy(ema_ref.at[:, pl.ds(first, width)], v_ref, v_sem)
    fetch.start()
    for shard in range(shards):
        t_ref[pl.ds(shard * t_rows, t_rows), :] = normal_rows(both_ref[shard, :t_rows, :])
        s_ref[pl.ds(shard * s_rows, s_rows), :] = normal_rows(both_ref[shard, t_rows:, :])
    fetch.wait()

    def fill(step, total):
        cols = pl.ds(pl.multiple_of(step * block, block), block)
        proto_f = v_ref[:, cols].astype(jnp.float32)
        unit = (proto_f * lax.rsqrt(jnp.sum(proto_f * proto_f, axis=0, keepdims=True))).astype(jnp.bfloat16)
        grown = jnp.exp(jnp.dot(t_ref[...], unit, preferred_element_type=jnp.float32) * (1.0 / TEMP_TEACHER))
        exp_ref[:, cols] = grown
        sums = jnp.sum(grown, axis=0, keepdims=True)
        return total + fold_lanes(sums)

    total = lax.fori_loop(0, steps, fill, jnp.zeros((1, LANES), jnp.float32))
    total = jnp.broadcast_to(jnp.sum(total, axis=1, keepdims=True), (1, LANES))
    scale_ref[...] = jnp.ones_like(scale_ref)
    await_all(n_dev)
    for it in range(SINK_ITERS):
        part_ref[...] = jnp.zeros_like(part_ref)
        lax.fori_loop(0, width // LANES, lambda s, c: sweep_at(s, c, exp_ref, scale_ref, col_ref, part_ref, n_proto), 0)
        send_ref[it] = jnp.zeros((8, LANES), jnp.float32)
        for group in range(groups):
            rows = pl.ds(group * LANES, LANES)
            send_ref[it, group:group + 1, :] = to_lanes(jnp.sum(part_ref[rows, :], axis=1, keepdims=True))
        send_ref[it, groups:groups + 1, :] = total
        sums = exchange(send_ref.at[it], recv_ref.at[it], send_sem.at[it], recv_sem.at[it], sizes, n_dev)
        crop = sums[:groups]
        if it == 0:
            whole = sums[groups:groups + 1]
            crop = crop * (whole * (1.0 / whole))
        scale = 1.0 / (crop * n_rows)
        for group in range(groups):
            rows = pl.ds(group * LANES, LANES)
            scale_ref[rows, :] = jnp.broadcast_to(to_rows(scale[group:group + 1]), (LANES, LANES))
        if it == SINK_ITERS - 1:
            row_ref[...] = jnp.zeros_like(row_ref)
            row_ref[:groups, :] = crop * scale * n_rows

    def finish(step, carry):
        cols = pl.ds(pl.multiple_of(step * LANES, LANES), LANES)
        target = exp_ref[:, cols] * scale_ref[...] * col_ref[:, cols] * n_rows
        high = target.astype(jnp.bfloat16)
        hi_ref[:, cols] = high
        lo_ref[:, cols] = (target - high.astype(jnp.float32)).astype(jnp.bfloat16)
        return carry

    lax.fori_loop(0, width // LANES, finish, 0)


def sweep_at(step, carry, exp_ref, scale_ref, col_ref, part_ref, n_proto):
    cols = pl.ds(pl.multiple_of(step * LANES, LANES), LANES)
    grown = exp_ref[:, cols]
    col = 1.0 / (jnp.sum(grown * scale_ref[...], axis=0, keepdims=True) * n_proto)
    col_ref[:, cols] = col
    part_ref[...] += grown * col
    return carry


def sinkhorn(both, ema_protos, sizes, n_proto, n_rows, width):
    shards, per_dev, depth = both.shape
    n_student = shards * per_dev - n_rows
    n_dev = 1
    for size in sizes:
        n_dev *= size
    vmem, hbm = pl.BlockSpec(memory_space=pltpu.VMEM), pl.BlockSpec(memory_space=pl.ANY)
    target = jax.ShapeDtypeStruct((n_rows, width), jnp.bfloat16)
    return pl.pallas_call(
        functools.partial(sink_kernel, sizes, n_proto, 512),
        out_shape=(target, target, jax.ShapeDtypeStruct((8, LANES), jnp.float32),
                   jax.ShapeDtypeStruct((n_student, depth), jnp.bfloat16)),
        in_specs=[vmem, hbm], out_specs=(vmem,) * 4,
        scratch_shapes=[
            pltpu.VMEM((n_rows, depth), jnp.bfloat16), pltpu.VMEM((depth, width), jnp.bfloat16),
            pltpu.VMEM((n_rows, width), jnp.float32), pltpu.VMEM((1, width), jnp.float32),
            pltpu.VMEM((n_rows, LANES), jnp.float32), pltpu.VMEM((n_rows, LANES), jnp.float32),
            pltpu.VMEM((SINK_ITERS, 8, LANES), jnp.float32), pltpu.VMEM((SINK_ITERS, n_dev, 8, LANES), jnp.float32),
            pltpu.SemaphoreType.DMA, pltpu.SemaphoreType.DMA((SINK_ITERS, n_dev)),
            pltpu.SemaphoreType.DMA((SINK_ITERS, n_dev))],
        compiler_params=pltpu.CompilerParams(collective_id=0, has_side_effects=True, vmem_limit_bytes=40 << 20),
        cost_estimate=pl.CostEstimate(flops=20 * 10 ** 9, bytes_accessed=12 << 20, transcendentals=n_rows * width),
    )(both, ema_protos)


def soft_kernel(rows, base_ref, s_ref, v_ref, hi_ref, lo_ref, exp_ref, part_ref, exp_u_ref, hi_u_ref, lo_u_ref):
    @pl.when(pl.program_id(0) == 0)
    def _():
        part_ref[...] = jnp.zeros_like(part_ref)
        exp_u_ref[...] = jnp.zeros_like(exp_u_ref)
        hi_u_ref[...] = jnp.zeros_like(hi_u_ref)
        lo_u_ref[...] = jnp.zeros_like(lo_u_ref)

    proto_f = v_ref[...].astype(jnp.float32)
    unit = (proto_f * lax.rsqrt(jnp.sum(proto_f * proto_f, axis=0, keepdims=True))).astype(jnp.bfloat16)
    across = (((1,), (1,)), ((), ()))
    hi_u_ref[...] += lax.dot_general(hi_ref[...], unit, across, preferred_element_type=jnp.float32)
    lo_u_ref[...] += lax.dot_general(lo_ref[...], unit, across, preferred_element_type=jnp.float32)

    def one(step, carry):
        at = pl.ds(pl.multiple_of(step * rows, rows), rows)
        logits = jnp.dot(s_ref[at, :], unit, preferred_element_type=jnp.float32) * (1.0 / TEMP_STUDENT)
        grown = jnp.exp(logits)
        part_ref[at, :] += fold_lanes(grown)
        low = grown.astype(jnp.bfloat16)
        exp_ref[at, :] = low
        exp_u_ref[at, :] += lax.dot_general(low, unit, across, preferred_element_type=jnp.float32)
        return carry

    lax.fori_loop(0, s_ref.shape[0] // rows, one, 0)


def soft_pass(base, s_all, protos, hi, lo):
    n_student, depth = s_all.shape
    n_rows, width = hi.shape
    block = 512
    whole = lambda shape: pl.BlockSpec(shape, lambda k, base_ref: (0, 0))
    cols = lambda height: pl.BlockSpec((height, block), lambda k, base_ref: (0, k))
    own = pl.BlockSpec((depth, block), lambda k, base_ref: (0, base_ref[0] * (width // block) + k))
    wide = lambda height, span: jax.ShapeDtypeStruct((height, span), jnp.float32)
    return pl.pallas_call(
        functools.partial(soft_kernel, 640),
        grid_spec=pltpu.PrefetchScalarGridSpec(
            num_scalar_prefetch=1, grid=(width // block,),
            in_specs=[whole((n_student, depth)), own, cols(n_rows), cols(n_rows)],
            out_specs=(cols(n_student), whole((n_student, LANES)), whole((n_student, depth)),
                       whole((n_rows, depth)), whole((n_rows, depth)))),
        out_shape=(jax.ShapeDtypeStruct((n_student, width), jnp.bfloat16), wide(n_student, LANES),
                   wide(n_student, depth), wide(n_rows, depth), wide(n_rows, depth)),
        compiler_params=pltpu.CompilerParams(dimension_semantics=('arbitrary',), vmem_limit_bytes=50 << 20),
        cost_estimate=pl.CostEstimate(flops=13 * 10 ** 9, bytes_accessed=35 << 20, transcendentals=n_student * width),
    )(base, s_all, protos, hi, lo)


def crop_weights(lines, per_dev, n_img):
    spot = (lax.broadcasted_iota(jnp.int32, (lines, LANES), 0) * LANES
            + lax.broadcasted_iota(jnp.int32, (lines, LANES), 1))
    is_global = lax.rem(spot, per_dev) < GLOBAL_CROPS * n_img
    return jnp.where(is_global, float(GLOBAL_CROPS - 1), float(GLOBAL_CROPS))


def line_kernel(sizes, n_img, part_ref, s_ref, hi_u_ref, lo_u_ref, sum_ref, weight_ref,
                line_ref, line_recv, line_send_sem, line_recv_sem):
    n_dev = 1
    for size in sizes:
        n_dev *= size
    shards = n_dev // sizes[0]
    n_student, depth = s_ref.shape
    per_dev = n_student // shards
    groups = n_student // LANES
    greet_all(sizes, n_dev)
    line_ref[...] = jnp.zeros_like(line_ref)
    for group in range(groups):
        rows = pl.ds(group * LANES, LANES)
        line_ref[group:group + 1, :] = to_lanes(jnp.sum(part_ref[rows, :], axis=1, keepdims=True))

    def view_sum(shard, hits):
        base = pl.multiple_of(shard * per_dev, n_img)
        views = [s_ref[pl.ds(base + view * n_img, n_img), :].astype(jnp.float32) for view in range(ALL_CROPS)]
        total = views[0]
        for view in views[1:]:
            total = total + view
        for crop in range(GLOBAL_CROPS):
            rows = pl.ds(pl.multiple_of((shard * GLOBAL_CROPS + crop) * n_img, n_img), n_img)
            hits = hits + (total - views[crop]) * (hi_u_ref[rows, :] + lo_u_ref[rows, :])
        return hits

    hits = lax.fori_loop(0, shards, view_sum, jnp.zeros((n_img, depth), jnp.float32))
    hits = jnp.sum(jnp.sum(hits, axis=1, keepdims=True), axis=0, keepdims=True)
    line_ref[groups:groups + 1, :] = jnp.broadcast_to(hits, (1, LANES))
    await_all(n_dev)
    sums = exchange(line_ref, line_recv, line_send_sem, line_recv_sem, sizes, n_dev)
    sum_ref[...] = sums
    lines = sums.shape[0]
    weight_ref[...] = crop_weights(lines, per_dev, n_img) / sums


def turn_factors(n_img, weight_ref, s_ref, soft_ref, pair_ref):
    n_student = s_ref.shape[0]
    for group in range(n_student // LANES):
        rows = pl.ds(group * LANES, LANES)
        turned = s_ref[rows, :].astype(jnp.float32).T
        soft_ref[:, rows] = (turned * weight_ref[group:group + 1, :]).astype(soft_ref.dtype)
    per_dev = ALL_CROPS * n_img
    pairs = []
    for shard in range(n_student // per_dev):
        views = [s_ref[pl.ds(shard * per_dev + view * n_img, n_img), :].astype(jnp.float32) for view in range(ALL_CROPS)]
        total = views[0]
        for view in views[1:]:
            total = total + view
        pairs += [total - views[crop] for crop in range(GLOBAL_CROPS)]
    per_tile = LANES // n_img
    for tile in range(len(pairs) // per_tile):
        rows = jnp.concatenate(pairs[tile * per_tile:(tile + 1) * per_tile], axis=0)
        pair_ref[:, pl.ds(tile * LANES, LANES)] = rows.T.astype(pair_ref.dtype)


def emb_kernel(sizes, n_img, factor, block, weight_ref, exp_u_ref, hi_u_ref, s_ref, exp_hbm, hi_hbm, protos_hbm,
               out_ref, own_ref,
               wide_ref, g_ref, near_recv, acc_ref, piece_recv, piece_ref, gathered, full_ref,
               soft_ref, pair_ref, exp_ref, hi_ref, v_ref,
               near_send_sem, near_recv_sem, piece_send_sem, piece_recv_sem, all_send_sem, all_recv_sem,
               exp_sem, hi_sem, v_sem):
    n_dev = 1
    for size in sizes:
        n_dev *= size
    chips = n_dev // 2
    shards = n_dev // sizes[0]
    n_student, depth = exp_u_ref.shape
    per_dev = n_student // shards
    groups = n_student // LANES
    mesh_type = pl.DeviceIdType.MESH
    me = my_place(sizes)
    core = lax.rem(me, 2)
    chip = me // 2
    greet_all(sizes, n_dev)
    width = own_ref.shape[1]
    steps = width // block

    def fetch(step):
        cols = pl.ds(pl.multiple_of(step * block, block), block)
        slot = lax.rem(step, 2)
        return pltpu.make_async_copy(exp_hbm.at[:, cols], exp_ref.at[slot], exp_sem.at[slot])

    first = pl.multiple_of(lax.rem(me, shards) * width, width)
    get_v = pltpu.make_async_copy(protos_hbm.at[:, pl.ds(first, width)], v_ref, v_sem)
    get_hi = pltpu.make_async_copy(hi_hbm, hi_ref, hi_sem)
    get_v.start()
    get_hi.start()
    fetch(0).start()

    def grad_block(step, carry):
        cols = pl.ds(pl.multiple_of(step * block, block), block)

        @pl.when(step + 1 < steps)
        def _():
            fetch(step + 1).start()

        fetch(step).wait()
        g_unit = jnp.dot(soft_ref[...], exp_ref[lax.rem(step, 2)], preferred_element_type=jnp.float32)
        g_unit = (g_unit - jnp.dot(pair_ref[...], hi_ref[:, cols], preferred_element_type=jnp.float32)) * factor
        proto_f = v_ref[:, cols].astype(jnp.float32)
        inv_col = lax.rsqrt(jnp.sum(proto_f * proto_f, axis=0, keepdims=True))
        unit = proto_f * inv_col
        own_ref[:, cols] = (g_unit - unit * jnp.sum(unit * g_unit, axis=0, keepdims=True)) * inv_col
        return carry

    weight = weight_ref[...]
    for group in range(groups):
        rows = pl.ds(group * LANES, LANES)
        wide_ref[rows, :] = jnp.broadcast_to(to_rows(weight[group:group + 1]), (LANES, LANES))

    def combine(shard, carry):
        to_core = lax.rem(shard, 2)
        base = pl.multiple_of(shard * per_dev, n_img)
        land = pl.multiple_of((shard // 2) * per_dev, n_img)
        tops = [hi_u_ref[pl.ds(pl.multiple_of((shard * GLOBAL_CROPS + crop) * n_img, n_img), n_img), :]
                for crop in range(GLOBAL_CROPS)]
        both = tops[0] + tops[1]
        for view in range(ALL_CROPS):
            rows = pl.ds(base + view * n_img, n_img)
            target = both - tops[view] if view < GLOBAL_CROPS else both
            wide = wide_ref[rows, :]
            soft = exp_u_ref[rows, :] * jnp.concatenate([wide, wide], axis=1)
            g_ref[to_core, pl.ds(land + view * n_img, n_img), :] = (soft - target) * factor
        return carry

    lax.fori_loop(0, shards, combine, 0)
    await_all(n_dev)
    near = pltpu.make_async_remote_copy(
        src_ref=g_ref.at[1 - core], dst_ref=near_recv, send_sem=near_send_sem, recv_sem=near_recv_sem,
        device_id=place_of(chip * 2 + (1 - core), sizes), device_id_type=mesh_type)
    near.start()
    turn_factors(n_img, weight_ref, s_ref, soft_ref, pair_ref)
    get_v.wait()
    get_hi.wait()
    near.wait()
    acc_ref[...] = g_ref[core] + near_recv[...]
    piece = acc_ref.shape[0] // chips
    copies = []
    for step in range(1, chips):
        peer = lax.rem(chip + step, chips)
        copy = pltpu.make_async_remote_copy(
            src_ref=acc_ref.at[pl.ds(pl.multiple_of(peer * piece, n_img), piece)], dst_ref=piece_recv.at[step],
            send_sem=piece_send_sem.at[step], recv_sem=piece_recv_sem.at[step],
            device_id=place_of(peer * 2 + core, sizes), device_id_type=mesh_type)
        copy.start()
        copies.append(copy)
    lax.fori_loop(0, steps // 2, grad_block, 0)
    total = acc_ref[pl.ds(pl.multiple_of(chip * piece, n_img), piece), :]
    for step in range(1, chips):
        copies[step - 1].wait()
        total = total + piece_recv[step]
    piece_ref[...] = total
    copies = []
    for step in range(1, chips):
        peer = lax.rem(chip + step, chips)
        copy = pltpu.make_async_remote_copy(
            src_ref=piece_ref, dst_ref=gathered.at[step], send_sem=all_send_sem.at[step], recv_sem=all_recv_sem.at[step],
            device_id=place_of(peer * 2 + core, sizes), device_id_type=mesh_type)
        copy.start()
        copies.append(copy)
    full_ref[pl.ds(pl.multiple_of(chip * piece, n_img), piece), :] = total
    lax.fori_loop(steps // 2, steps, grad_block, 0)
    for step in range(1, chips):
        copies[step - 1].wait()
        owner = lax.rem(chip + chips - step, chips)
        full_ref[pl.ds(pl.multiple_of(owner * piece, n_img), piece), :] = gathered[step]
    for base in range(0, full_ref.shape[0], per_dev):
        for view in range(ALL_CROPS):
            for lane in range(depth // LANES):
                at = pl.ds(lane * LANES, LANES)
                rows = pl.ds(base + view, n_img, stride=ALL_CROPS)
                out_ref[lane, rows, :] = full_ref[pl.ds(base + view * n_img, n_img), at]


def crop_lines(part, s_all, hi_u, lo_u, sizes, n_img):
    lines = (part.shape[0] // LANES // 8 + 1) * 8
    n_dev = 1
    for size in sizes:
        n_dev *= size
    vmem = pl.BlockSpec(memory_space=pltpu.VMEM)
    line = jax.ShapeDtypeStruct((lines, LANES), jnp.float32)
    return pl.pallas_call(
        functools.partial(line_kernel, sizes, n_img), out_shape=(line, line), in_specs=[vmem] * 4, out_specs=(vmem,) * 2,
        scratch_shapes=[
            pltpu.VMEM((lines, LANES), jnp.float32), pltpu.VMEM((n_dev, lines, LANES), jnp.float32),
            pltpu.SemaphoreType.DMA((n_dev,)), pltpu.SemaphoreType.DMA((n_dev,))],
        compiler_params=pltpu.CompilerParams(collective_id=1, has_side_effects=True, vmem_limit_bytes=24 << 20),
        cost_estimate=pl.CostEstimate(flops=5 * 10 ** 9, bytes_accessed=4 << 20, transcendentals=0),
    )(part, s_all, hi_u, lo_u)


def emb_grads(weight, exp_u, hi_u, s_all, exp_lo, hi, protos, sizes, n_img, factor):
    n_student, depth = exp_u.shape
    n_rows, width = hi.shape
    block = 512
    n_dev = 1
    for size in sizes:
        n_dev *= size
    half, chips = n_student // 2, n_dev // 2
    vmem, hbm = pl.BlockSpec(memory_space=pltpu.VMEM), pl.BlockSpec(memory_space=pl.ANY)
    wide, low = jnp.float32, jnp.bfloat16
    dma = pltpu.SemaphoreType.DMA
    return pl.pallas_call(
        functools.partial(emb_kernel, sizes, n_img, factor, block),
        out_shape=(jax.ShapeDtypeStruct((depth // LANES, half, LANES), wide), jax.ShapeDtypeStruct((depth, width), wide)),
        in_specs=[vmem] * 4 + [hbm] * 3, out_specs=(vmem,) * 2,
        scratch_shapes=[
            pltpu.VMEM((n_student, LANES), wide), pltpu.VMEM((2, half, depth), wide), pltpu.VMEM((half, depth), wide),
            pltpu.VMEM((half, depth), wide), pltpu.VMEM((chips, half // chips, depth), wide),
            pltpu.VMEM((half // chips, depth), wide), pltpu.VMEM((chips, half // chips, depth), wide),
            pltpu.VMEM((half, depth), wide),
            pltpu.VMEM((depth, n_student), low), pltpu.VMEM((depth, n_rows), low),
            pltpu.VMEM((2, n_student, block), low), pltpu.VMEM((n_rows, width), low), pltpu.VMEM((depth, width), low),
            dma, dma, dma((chips,)), dma((chips,)), dma((chips,)), dma((chips,)), dma((2,)), dma, dma],
        compiler_params=pltpu.CompilerParams(collective_id=2, has_side_effects=True, vmem_limit_bytes=56 << 20),
        cost_estimate=pl.CostEstimate(flops=30 * 10 ** 9, bytes_accessed=40 << 20, transcendentals=0),
    )(weight, exp_u, hi_u, s_all, exp_lo, hi, protos)


def solution(mesh):
    vp_size = mesh.shape['vp']
    dp_size = mesh.shape['dp']
    sizes = (vp_size, dp_size // 4, 2, 2)
    fine = Mesh(mesh.devices.reshape(sizes), AXES)
    data = ('y', 'x', 'core')

    def local_step(student_x, teacher_x, w_in, b_in, w_mid, b_mid, w_out, b_out, protos,
                   ema_w_in, ema_b_in, ema_w_mid, ema_b_mid, ema_w_out, ema_b_out, ema_protos):
        n_img = student_x.shape[0] // ALL_CROPS
        part = protos.shape[1] // dp_size
        n_proto = protos.shape[1] * vp_size
        n_rows = GLOBAL_CROPS * n_img * dp_size
        n_student = ALL_CROPS * n_img * dp_size
        core = lax.axis_index('core')
        data_idx = (lax.axis_index('y') * 2 + lax.axis_index('x')) * 2 + core
        base = data_idx.reshape(1)

        rows_b = (ema_b_in, ema_b_mid, b_in, b_mid, ema_b_out, b_out)
        starts = []
        for row in rows_b:
            starts.append(starts[-1] + width if starts else 0)
            width = row.shape[0]
        total = starts[-1] + width
        biases = sum(jnp.pad(row.astype(jnp.float32), (start, total - start - row.shape[0]))
                     for row, start in zip(rows_b, starts))[None]
        offsets = (starts[0], starts[1], starts[4], starts[2], starts[3], starts[5])
        both = head_pass(teacher_x, student_x, biases, offsets, (ema_w_in, ema_w_mid, ema_w_out), (w_in, w_mid, w_out))
        both = gather_rows(both[None], data)
        both, own_x = lax.optimization_barrier((both, student_x))
        half_wide = gather_rows(own_x, ('y', 'x'))

        q_hi, q_lo, q_row, s_all = sinkhorn(both, ema_protos, sizes, n_proto, n_rows, part)
        exp_lo, row_part, exp_u, hi_u, lo_u = soft_pass(base, s_all, protos, q_hi, q_lo)
        scale = 1.0 / (n_img * dp_size * GLOBAL_CROPS * (ALL_CROPS - 1))
        factor = scale / TEMP_STUDENT
        sums, weight = crop_lines(row_part, s_all, hi_u, lo_u, sizes, n_img)
        g_emb, g_own = emb_grads(weight, exp_u, hi_u, s_all, exp_lo, q_hi, protos, sizes, n_img, factor)
        g_emb = jnp.concatenate([g_emb[lane] for lane in range(g_emb.shape[0])], axis=1)
        g_own, half_wide = lax.optimization_barrier((g_own, half_wide))
        g_protos = lax.all_gather(g_own, data, axis=1, tiled=True)

        per_view = q_row[:n_rows // LANES].reshape(dp_size, GLOBAL_CROPS, n_img)
        pad = jnp.pad(per_view, ((0, 0), (0, ALL_CROPS - GLOBAL_CROPS), (0, 0)))
        t_row = (jnp.sum(per_view, axis=1, keepdims=True) - pad).reshape(-1)
        row_line = sums.reshape(-1)[:n_student]
        hits = sums[n_student // LANES, 0]
        loss = (jnp.sum(t_row * jnp.log(row_line)) - hits / TEMP_STUDENT) * scale

        hid_one, slope_one, half_x = mlp_layer(half_wide, w_in, biases, offsets[3])
        hid_two, slope_two = mlp_layer(hid_one, w_mid, biases, offsets[4])
        grads = mlp_backward(g_emb, half_x, (hid_one, slope_one, hid_two, slope_two), w_mid, w_out, b_out)
        other = lambda g: lax.ppermute(g, 'core', [(0, 1), (1, 0)])
        got_mid, got_in = other(grads[2]), other(grads[0])
        sum_mid = grads[2] + got_mid
        small = jnp.concatenate([grads[1], grads[3], grads[5]])
        small, g_out, sum_mid = lax.optimization_barrier((small, grads[4], sum_mid))
        got_small, got_out = other(small), other(g_out)
        sum_in = grads[0] + got_in
        biases = small + got_small
        b_grads = jnp.split(biases, [b_in.shape[0], b_in.shape[0] + b_mid.shape[0]])
        return (loss, sum_in, b_grads[0], sum_mid, b_grads[1], g_out + got_out, b_grads[2], g_protos)

    by_rows = P(data, None)
    by_cols = P(None, 'vp')
    replicated = P()
    head_specs = (replicated,) * 6
    in_specs = (by_rows, by_rows) + head_specs + (by_cols,) + head_specs + (by_cols,)
    out_specs = (replicated,) * 7 + (by_cols,)
    return jax.shard_map(local_step, mesh=fine, in_specs=in_specs, out_specs=out_specs, check_vma=False)
```

```python
import functools

import jax
import jax.numpy as jnp
from jax import lax
from jax.experimental import pallas as pl
from jax.experimental.pallas import tpu as pltpu
from jax.sharding import Mesh, PartitionSpec as P

ALL_CROPS = 10
GLOBAL_CROPS = 2
SINK_ITERS = 3
TEMP_STUDENT = 0.1
TEMP_TEACHER = 0.04


def layer_kernel(rows, feats_ref, w_ref, bias_ref, hid_ref, slope_ref, *narrow):
    if narrow:
        @pl.when(pl.program_id(0) == 0)
        def _():
            narrow[0][...] = feats_ref[...].astype(jnp.bfloat16)
        feats_ref = narrow[0]

    def one(step, carry):
        at = pl.ds(pl.multiple_of(step * rows, rows), rows)
        pre = jnp.dot(feats_ref[at, :], w_ref[...], preferred_element_type=jnp.float32) + bias_ref[...]
        cdf = 0.5 * (1.0 + lax.erf(pre * 0.7071067811865476))
        hid_ref[at, :] = (pre * cdf).astype(hid_ref.dtype)
        slope_ref[at, :] = cdf + pre * jnp.exp(-0.5 * pre * pre) * 0.3989422804014327
        return carry

    lax.fori_loop(0, feats_ref.shape[0] // rows, one, 0)


def mlp_layer(feats, w, biases, offset):
    count, fan_in = feats.shape
    width = w.shape[1]
    block = 512
    whole = pl.BlockSpec((count, fan_in), lambda k: (0, 0))
    out = pl.BlockSpec((count, block), lambda k: (0, k))
    narrow = feats.dtype != jnp.bfloat16
    shapes = [jax.ShapeDtypeStruct((count, width), jnp.bfloat16), jax.ShapeDtypeStruct((count, width), jnp.float32)]
    return pl.pallas_call(
        functools.partial(layer_kernel, count // 4), grid=(width // block,),
        out_shape=tuple(shapes + [jax.ShapeDtypeStruct((count, fan_in), jnp.bfloat16)] * narrow),
        in_specs=[whole, pl.BlockSpec((fan_in, block), lambda k: (0, k)),
                  pl.BlockSpec((1, block), lambda k: (0, offset // block + k))],
        out_specs=tuple([out, out] + [whole] * narrow),
        compiler_params=pltpu.CompilerParams(dimension_semantics=('arbitrary',), vmem_limit_bytes=56 << 20),
        cost_estimate=pl.CostEstimate(flops=2 * count * fan_in * width, bytes_accessed=30 << 20,
                                      transcendentals=2 * count * width))(feats, w, biases)


def mlp_backward(g_emb, feats, saved, w_mid, w_out, b_out):
    hid_one, slope_one, hid_two, slope_two = saved
    proj = jnp.dot(hid_two, w_out, preferred_element_type=jnp.float32) + b_out.astype(jnp.float32)
    inv_norm = lax.rsqrt(jnp.sum(proj * proj, axis=-1, keepdims=True))
    unit = proj * inv_norm
    g_proj = (g_emb - unit * jnp.sum(unit * g_emb, axis=-1, keepdims=True)) * inv_norm
    g_proj_lo = g_proj.astype(jnp.bfloat16)
    g_w_out = jnp.einsum('nh,nb->hb', hid_two, g_proj_lo, preferred_element_type=jnp.float32)
    g_hid_two = jnp.einsum('nb,hb->nh', g_proj_lo, w_out, preferred_element_type=jnp.float32)
    g_pre_two = g_hid_two.astype(jnp.bfloat16).astype(jnp.float32) * slope_two
    g_pre_two_lo = g_pre_two.astype(jnp.bfloat16)
    g_w_mid = jnp.einsum('ng,nh->gh', hid_one, g_pre_two_lo, preferred_element_type=jnp.float32)
    g_hid_one = jnp.einsum('nh,gh->ng', g_pre_two_lo, w_mid, preferred_element_type=jnp.float32)
    g_pre_one = g_hid_one.astype(jnp.bfloat16).astype(jnp.float32) * slope_one
    g_w_in = jnp.einsum('nf,nh->fh', feats, g_pre_one.astype(jnp.bfloat16), preferred_element_type=jnp.float32)
    return (g_w_in, jnp.sum(g_pre_one, axis=0), g_w_mid, jnp.sum(g_pre_two, axis=0), g_w_out, jnp.sum(g_proj, axis=0))


def col_normalize(protos):
    proto_f = protos.astype(jnp.float32)
    inv_col = lax.rsqrt(jnp.sum(proto_f * proto_f, axis=0, keepdims=True))
    unit = proto_f * inv_col
    return unit.astype(jnp.bfloat16), unit, inv_col


def col_normalize_backward(g_unit, unit, inv_col):
    return (g_unit - unit * jnp.sum(unit * g_unit, axis=0, keepdims=True)) * inv_col


def gather_rows(vals, axis_name):
    return lax.all_gather(vals.astype(jnp.float32), axis_name, axis=0, tiled=True)


LANES = 128
AXES = ('vp', 'y', 'x', 'core')


def my_place(sizes):
    flat = 0
    for name, size in zip(AXES, sizes):
        flat = flat * size + lax.axis_index(name)
    return flat


def place_of(flat, sizes):
    coords = []
    for size in reversed(sizes):
        coords.append(lax.rem(flat, size))
        flat = flat // size
    return tuple(reversed(coords))


def greet_all(sizes, n_dev):
    barrier = pltpu.get_barrier_semaphore()
    me = my_place(sizes)
    for step in range(1, n_dev):
        peer = lax.rem(me + step, n_dev)
        pl.semaphore_signal(barrier, inc=1, device_id=place_of(peer, sizes), device_id_type=pl.DeviceIdType.MESH)


def await_all(n_dev):
    pl.semaphore_wait(pltpu.get_barrier_semaphore(), n_dev - 1)


def exchange(send_ref, recv_ref, send_sem, recv_sem, sizes, n_dev):
    me = my_place(sizes)
    copies = []
    for step in range(1, n_dev):
        peer = lax.rem(me + step, n_dev)
        copy = pltpu.make_async_remote_copy(
            src_ref=send_ref, dst_ref=recv_ref.at[step], send_sem=send_sem.at[step], recv_sem=recv_sem.at[step],
            device_id=place_of(peer, sizes), device_id_type=pl.DeviceIdType.MESH)
        copy.start()
        copies.append(copy)
    for copy in copies:
        copy.wait()
    total = send_ref[...]
    for step in range(1, n_dev):
        total = total + recv_ref[step]
    return total


def eye_mask():
    rows = lax.broadcasted_iota(jnp.int32, (LANES, LANES), 0)
    cols = lax.broadcasted_iota(jnp.int32, (LANES, LANES), 1)
    return rows == cols


def to_lanes(column):
    return jnp.sum(jnp.where(eye_mask(), jnp.broadcast_to(column, (LANES, LANES)), 0.0), axis=0, keepdims=True)


def to_rows(line):
    return jnp.sum(jnp.where(eye_mask(), jnp.broadcast_to(line, (LANES, LANES)), 0.0), axis=1, keepdims=True)


def fold_lanes(tile):
    total = tile[:, :LANES]
    for start in range(LANES, tile.shape[1], LANES):
        total = total + tile[:, start:start + LANES]
    return total


def head_kernel(chunk, offsets, tx_ref, sx_ref, bias_ref, *refs):
    weights, (out_ref,), bufs, (hid_one, hid_two, proj_ref, sems) = refs[:6], refs[6:7], refs[7:13], refs[13:]
    t_rows = tx_ref.shape[0]
    order = (0, 3, 1, 4, 2, 5)
    slot = {}
    used = 0
    for which in order:
        slot[which] = used
        span = min(chunk, weights[which].shape[1])
        for step in range(weights[which].shape[1] // span):
            cols = pl.ds(step * span, span)
            pltpu.make_async_copy(weights[which].at[:, cols], bufs[which].at[:, cols], sems.at[used]).start()
            used += 1

    def layer(which, feats, store):
        buf = bufs[which]
        span = min(chunk, buf.shape[1])

        def one(step, carry):
            cols = pl.ds(pl.multiple_of(step * span, span), span)
            pltpu.make_async_copy(weights[which].at[:, cols], buf.at[:, cols], sems.at[slot[which] + step]).wait()
            bias_at = pl.ds(pl.multiple_of(offsets[which] + step * span, LANES), span)
            store(cols, jnp.dot(feats[...], buf[:, cols], preferred_element_type=jnp.float32) + bias_ref[:, bias_at])
            return carry

        lax.fori_loop(0, buf.shape[1] // span, one, 0)

    def hidden(ref, rows):
        def store(cols, pre):
            ref[rows, cols] = (0.5 * pre * (1.0 + lax.erf(pre * 0.7071067811865476))).astype(ref.dtype)
        return store

    def project(rows):
        def store(cols, proj):
            for lane in range(proj_ref.shape[0]):
                proj_ref[lane, rows, :] = proj[:, lane * LANES:(lane + 1) * LANES]
        return store

    ours, theirs = pl.ds(t_rows, sx_ref.shape[0]), pl.ds(0, t_rows)
    layer(0, tx_ref, hidden(hid_one, theirs))
    layer(3, sx_ref, hidden(hid_one, ours))
    layer(1, hid_one.at[theirs], hidden(hid_two, theirs))
    layer(4, hid_one.at[ours], hidden(hid_two, ours))
    layer(2, hid_two.at[theirs], project(theirs))
    layer(5, hid_two.at[ours], project(ours))
    for start, views, count in ((0, GLOBAL_CROPS, t_rows), (t_rows, ALL_CROPS, sx_ref.shape[0])):
        n_img = count // views
        for view in range(views):
            for lane in range(proj_ref.shape[0]):
                at = pl.ds(lane * LANES, LANES)
                rows = pl.ds(start + view, n_img, stride=views)
                out_ref[pl.ds(start + view * n_img, n_img), at] = proj_ref[lane, rows, :]


def head_pass(own_tx, own_x, biases, offsets, teacher, student):
    hidden = student[0].shape[1]
    weights = teacher + student
    rows = own_tx.shape[0] + own_x.shape[0]
    vmem, hbm = pl.BlockSpec(memory_space=pltpu.VMEM), pl.BlockSpec(memory_space=pl.ANY)
    return pl.pallas_call(
        functools.partial(head_kernel, 512, offsets),
        out_shape=jax.ShapeDtypeStruct((rows, student[2].shape[1]), jnp.float32),
        in_specs=[vmem] * 3 + [hbm] * 6, out_specs=vmem,
        scratch_shapes=[pltpu.VMEM(w.shape, w.dtype) for w in weights]
        + [pltpu.VMEM((rows, hidden), jnp.bfloat16)] * 2 + [pltpu.VMEM((student[2].shape[1] // LANES, rows, LANES), jnp.float32)] + [pltpu.SemaphoreType.DMA((24,))],
        compiler_params=pltpu.CompilerParams(vmem_limit_bytes=56 << 20),
        cost_estimate=pl.CostEstimate(flops=10 ** 10, bytes_accessed=34 << 20, transcendentals=rows * hidden * 2),
    )(own_tx, own_x, biases, *weights)


def normal_rows(proj):
    return (proj * lax.rsqrt(jnp.sum(proj * proj, axis=-1, keepdims=True))).astype(jnp.bfloat16)


def sink_kernel(sizes, n_proto, block, both_ref, ema_ref, hi_ref, lo_ref, row_ref, s_ref,
                t_ref, v_ref, exp_ref, col_ref, scale_ref, part_ref, send_ref, recv_ref, v_sem, send_sem, recv_sem):
    n_dev = 1
    for size in sizes:
        n_dev *= size
    n_rows, width = exp_ref.shape
    groups = n_rows // LANES
    steps = width // block
    shards, per_dev, _ = both_ref.shape
    t_rows = n_rows // shards
    s_rows = per_dev - t_rows
    greet_all(sizes, n_dev)
    first = pl.multiple_of(lax.rem(my_place(sizes), shards) * width, width)
    fetch = pltpu.make_async_copy(ema_ref.at[:, pl.ds(first, width)], v_ref, v_sem)
    fetch.start()
    for shard in range(shards):
        t_ref[pl.ds(shard * t_rows, t_rows), :] = normal_rows(both_ref[shard, :t_rows, :])
        s_ref[pl.ds(shard * s_rows, s_rows), :] = normal_rows(both_ref[shard, t_rows:, :])
    fetch.wait()

    def fill(step, total):
        cols = pl.ds(pl.multiple_of(step * block, block), block)
        proto_f = v_ref[:, cols].astype(jnp.float32)
        unit = (proto_f * lax.rsqrt(jnp.sum(proto_f * proto_f, axis=0, keepdims=True))).astype(jnp.bfloat16)
        grown = jnp.exp(jnp.dot(t_ref[...], unit, preferred_element_type=jnp.float32) * (1.0 / TEMP_TEACHER))
        exp_ref[:, cols] = grown
        sums = jnp.sum(grown, axis=0, keepdims=True)
        return total + fold_lanes(sums)

    total = lax.fori_loop(0, steps, fill, jnp.zeros((1, LANES), jnp.float32))
    total = jnp.broadcast_to(jnp.sum(total, axis=1, keepdims=True), (1, LANES))
    scale_ref[...] = jnp.ones_like(scale_ref)
    await_all(n_dev)
    for it in range(SINK_ITERS):
        part_ref[...] = jnp.zeros_like(part_ref)
        lax.fori_loop(0, width // LANES, lambda s, c: sweep_at(s, c, exp_ref, scale_ref, col_ref, part_ref, n_proto), 0)
        send_ref[it] = jnp.zeros((8, LANES), jnp.float32)
        for group in range(groups):
            rows = pl.ds(group * LANES, LANES)
            send_ref[it, group:group + 1, :] = to_lanes(jnp.sum(part_ref[rows, :], axis=1, keepdims=True))
        send_ref[it, groups:groups + 1, :] = total
        sums = exchange(send_ref.at[it], recv_ref.at[it], send_sem.at[it], recv_sem.at[it], sizes, n_dev)
        crop = sums[:groups]
        if it == 0:
            whole = sums[groups:groups + 1]
            crop = crop * (whole * (1.0 / whole))
        scale = 1.0 / (crop * n_rows)
        for group in range(groups):
            rows = pl.ds(group * LANES, LANES)
            scale_ref[rows, :] = jnp.broadcast_to(to_rows(scale[group:group + 1]), (LANES, LANES))
        if it == SINK_ITERS - 1:
            row_ref[...] = jnp.zeros_like(row_ref)
            row_ref[:groups, :] = crop * scale * n_rows

    def finish(step, carry):
        cols = pl.ds(pl.multiple_of(step * LANES, LANES), LANES)
        target = exp_ref[:, cols] * scale_ref[...] * col_ref[:, cols] * n_rows
        high = target.astype(jnp.bfloat16)
        hi_ref[:, cols] = high
        lo_ref[:, cols] = (target - high.astype(jnp.float32)).astype(jnp.bfloat16)
        return carry

    lax.fori_loop(0, width // LANES, finish, 0)


def sweep_at(step, carry, exp_ref, scale_ref, col_ref, part_ref, n_proto):
    cols = pl.ds(pl.multiple_of(step * LANES, LANES), LANES)
    grown = exp_ref[:, cols]
    col = 1.0 / (jnp.sum(grown * scale_ref[...], axis=0, keepdims=True) * n_proto)
    col_ref[:, cols] = col
    part_ref[...] += grown * col
    return carry


def sinkhorn(both, ema_protos, sizes, n_proto, n_rows, width):
    shards, per_dev, depth = both.shape
    n_student = shards * per_dev - n_rows
    n_dev = 1
    for size in sizes:
        n_dev *= size
    vmem, hbm = pl.BlockSpec(memory_space=pltpu.VMEM), pl.BlockSpec(memory_space=pl.ANY)
    target = jax.ShapeDtypeStruct((n_rows, width), jnp.bfloat16)
    return pl.pallas_call(
        functools.partial(sink_kernel, sizes, n_proto, 512),
        out_shape=(target, target, jax.ShapeDtypeStruct((8, LANES), jnp.float32),
                   jax.ShapeDtypeStruct((n_student, depth), jnp.bfloat16)),
        in_specs=[vmem, hbm], out_specs=(vmem,) * 4,
        scratch_shapes=[
            pltpu.VMEM((n_rows, depth), jnp.bfloat16), pltpu.VMEM((depth, width), jnp.bfloat16),
            pltpu.VMEM((n_rows, width), jnp.float32), pltpu.VMEM((1, width), jnp.float32),
            pltpu.VMEM((n_rows, LANES), jnp.float32), pltpu.VMEM((n_rows, LANES), jnp.float32),
            pltpu.VMEM((SINK_ITERS, 8, LANES), jnp.float32), pltpu.VMEM((SINK_ITERS, n_dev, 8, LANES), jnp.float32),
            pltpu.SemaphoreType.DMA, pltpu.SemaphoreType.DMA((SINK_ITERS, n_dev)),
            pltpu.SemaphoreType.DMA((SINK_ITERS, n_dev))],
        compiler_params=pltpu.CompilerParams(collective_id=0, has_side_effects=True, vmem_limit_bytes=40 << 20),
        cost_estimate=pl.CostEstimate(flops=20 * 10 ** 9, bytes_accessed=12 << 20, transcendentals=n_rows * width),
    )(both, ema_protos)


def soft_kernel(rows, base_ref, s_ref, v_ref, hi_ref, lo_ref, exp_ref, part_ref, exp_u_ref, hi_u_ref, lo_u_ref):
    @pl.when(pl.program_id(0) == 0)
    def _():
        part_ref[...] = jnp.zeros_like(part_ref)
        exp_u_ref[...] = jnp.zeros_like(exp_u_ref)
        hi_u_ref[...] = jnp.zeros_like(hi_u_ref)
        lo_u_ref[...] = jnp.zeros_like(lo_u_ref)

    proto_f = v_ref[...].astype(jnp.float32)
    unit = (proto_f * lax.rsqrt(jnp.sum(proto_f * proto_f, axis=0, keepdims=True))).astype(jnp.bfloat16)
    across = (((1,), (1,)), ((), ()))
    hi_u_ref[...] += lax.dot_general(hi_ref[...], unit, across, preferred_element_type=jnp.float32)
    lo_u_ref[...] += lax.dot_general(lo_ref[...], unit, across, preferred_element_type=jnp.float32)

    def one(step, carry):
        at = pl.ds(pl.multiple_of(step * rows, rows), rows)
        logits = jnp.dot(s_ref[at, :], unit, preferred_element_type=jnp.float32) * (1.0 / TEMP_STUDENT)
        grown = jnp.exp(logits)
        part_ref[at, :] += fold_lanes(grown)
        low = grown.astype(jnp.bfloat16)
        exp_ref[at, :] = low
        exp_u_ref[at, :] += lax.dot_general(low, unit, across, preferred_element_type=jnp.float32)
        return carry

    lax.fori_loop(0, s_ref.shape[0] // rows, one, 0)


def soft_pass(base, s_all, protos, hi, lo):
    n_student, depth = s_all.shape
    n_rows, width = hi.shape
    block = 512
    whole = lambda shape: pl.BlockSpec(shape, lambda k, base_ref: (0, 0))
    cols = lambda height: pl.BlockSpec((height, block), lambda k, base_ref: (0, k))
    own = pl.BlockSpec((depth, block), lambda k, base_ref: (0, base_ref[0] * (width // block) + k))
    wide = lambda height, span: jax.ShapeDtypeStruct((height, span), jnp.float32)
    return pl.pallas_call(
        functools.partial(soft_kernel, 640),
        grid_spec=pltpu.PrefetchScalarGridSpec(
            num_scalar_prefetch=1, grid=(width // block,),
            in_specs=[whole((n_student, depth)), own, cols(n_rows), cols(n_rows)],
            out_specs=(cols(n_student), whole((n_student, LANES)), whole((n_student, depth)),
                       whole((n_rows, depth)), whole((n_rows, depth)))),
        out_shape=(jax.ShapeDtypeStruct((n_student, width), jnp.bfloat16), wide(n_student, LANES),
                   wide(n_student, depth), wide(n_rows, depth), wide(n_rows, depth)),
        compiler_params=pltpu.CompilerParams(dimension_semantics=('arbitrary',), vmem_limit_bytes=50 << 20),
        cost_estimate=pl.CostEstimate(flops=13 * 10 ** 9, bytes_accessed=35 << 20, transcendentals=n_student * width),
    )(base, s_all, protos, hi, lo)


def crop_weights(lines, per_dev, n_img):
    spot = (lax.broadcasted_iota(jnp.int32, (lines, LANES), 0) * LANES
            + lax.broadcasted_iota(jnp.int32, (lines, LANES), 1))
    is_global = lax.rem(spot, per_dev) < GLOBAL_CROPS * n_img
    return jnp.where(is_global, float(GLOBAL_CROPS - 1), float(GLOBAL_CROPS))


def line_kernel(sizes, n_img, part_ref, s_ref, hi_u_ref, lo_u_ref, sum_ref, weight_ref,
                line_ref, line_recv, line_send_sem, line_recv_sem):
    n_dev = 1
    for size in sizes:
        n_dev *= size
    shards = n_dev // sizes[0]
    n_student, depth = s_ref.shape
    per_dev = n_student // shards
    groups = n_student // LANES
    greet_all(sizes, n_dev)
    line_ref[...] = jnp.zeros_like(line_ref)
    for group in range(groups):
        rows = pl.ds(group * LANES, LANES)
        line_ref[group:group + 1, :] = to_lanes(jnp.sum(part_ref[rows, :], axis=1, keepdims=True))

    def view_sum(shard, hits):
        base = pl.multiple_of(shard * per_dev, n_img)
        views = [s_ref[pl.ds(base + view * n_img, n_img), :].astype(jnp.float32) for view in range(ALL_CROPS)]
        total = views[0]
        for view in views[1:]:
            total = total + view
        for crop in range(GLOBAL_CROPS):
            rows = pl.ds(pl.multiple_of((shard * GLOBAL_CROPS + crop) * n_img, n_img), n_img)
            hits = hits + (total - views[crop]) * (hi_u_ref[rows, :] + lo_u_ref[rows, :])
        return hits

    hits = lax.fori_loop(0, shards, view_sum, jnp.zeros((n_img, depth), jnp.float32))
    hits = jnp.sum(jnp.sum(hits, axis=1, keepdims=True), axis=0, keepdims=True)
    line_ref[groups:groups + 1, :] = jnp.broadcast_to(hits, (1, LANES))
    await_all(n_dev)
    sums = exchange(line_ref, line_recv, line_send_sem, line_recv_sem, sizes, n_dev)
    sum_ref[...] = sums
    lines = sums.shape[0]
    weight_ref[...] = crop_weights(lines, per_dev, n_img) / sums


def turn_factors(n_img, weight_ref, s_ref, soft_ref, pair_ref):
    n_student = s_ref.shape[0]
    for group in range(n_student // LANES):
        rows = pl.ds(group * LANES, LANES)
        turned = s_ref[rows, :].astype(jnp.float32).T
        soft_ref[:, rows] = (turned * weight_ref[group:group + 1, :]).astype(soft_ref.dtype)
    per_dev = ALL_CROPS * n_img
    pairs = []
    for shard in range(n_student // per_dev):
        views = [s_ref[pl.ds(shard * per_dev + view * n_img, n_img), :].astype(jnp.float32) for view in range(ALL_CROPS)]
        total = views[0]
        for view in views[1:]:
            total = total + view
        pairs += [total - views[crop] for crop in range(GLOBAL_CROPS)]
    per_tile = LANES // n_img
    for tile in range(len(pairs) // per_tile):
        rows = jnp.concatenate(pairs[tile * per_tile:(tile + 1) * per_tile], axis=0)
        pair_ref[:, pl.ds(tile * LANES, LANES)] = rows.T.astype(pair_ref.dtype)


def emb_kernel(sizes, n_img, factor, block, weight_ref, exp_u_ref, hi_u_ref, s_ref, exp_hbm, hi_hbm, protos_hbm,
               out_ref, early_ref, late_ref,
               wide_ref, g_ref, near_recv, acc_ref, piece_recv, piece_ref, gathered, full_ref,
               soft_ref, pair_ref, exp_ref, hi_ref, v_ref,
               near_send_sem, near_recv_sem, piece_send_sem, piece_recv_sem, all_send_sem, all_recv_sem,
               exp_sem, hi_sem, v_sem):
    n_dev = 1
    for size in sizes:
        n_dev *= size
    chips = n_dev // 2
    shards = n_dev // sizes[0]
    n_student, depth = exp_u_ref.shape
    per_dev = n_student // shards
    groups = n_student // LANES
    mesh_type = pl.DeviceIdType.MESH
    me = my_place(sizes)
    core = lax.rem(me, 2)
    chip = me // 2
    greet_all(sizes, n_dev)
    width = hi_hbm.shape[1]
    steps = width // block
    turn = early_ref.shape[1] // block

    def fetch(step):
        cols = pl.ds(pl.multiple_of(step * block, block), block)
        slot = lax.rem(step, 2)
        return pltpu.make_async_copy(exp_hbm.at[:, cols], exp_ref.at[slot], exp_sem.at[slot])

    first = pl.multiple_of(lax.rem(me, shards) * width, width)
    get_v = pltpu.make_async_copy(protos_hbm.at[:, pl.ds(first, width)], v_ref, v_sem)
    get_hi = pltpu.make_async_copy(hi_hbm, hi_ref, hi_sem)
    get_v.start()
    get_hi.start()
    fetch(0).start()

    def grad_block(dest_ref, start, step, carry):
        cols = pl.ds(pl.multiple_of(step * block, block), block)

        @pl.when(step + 1 < steps)
        def _():
            fetch(step + 1).start()

        fetch(step).wait()
        g_unit = jnp.dot(soft_ref[...], exp_ref[lax.rem(step, 2)], preferred_element_type=jnp.float32)
        g_unit = (g_unit - jnp.dot(pair_ref[...], hi_ref[:, cols], preferred_element_type=jnp.float32)) * factor
        proto_f = v_ref[:, cols].astype(jnp.float32)
        inv_col = lax.rsqrt(jnp.sum(proto_f * proto_f, axis=0, keepdims=True))
        unit = proto_f * inv_col
        land = pl.ds(pl.multiple_of((step - start) * block, block), block)
        dest_ref[:, land] = (g_unit - unit * jnp.sum(unit * g_unit, axis=0, keepdims=True)) * inv_col
        return carry

    weight = weight_ref[...]
    for group in range(groups):
        rows = pl.ds(group * LANES, LANES)
        wide_ref[rows, :] = jnp.broadcast_to(to_rows(weight[group:group + 1]), (LANES, LANES))

    def combine(shard, carry):
        to_core = lax.rem(shard, 2)
        base = pl.multiple_of(shard * per_dev, n_img)
        land = pl.multiple_of((shard // 2) * per_dev, n_img)
        tops = [hi_u_ref[pl.ds(pl.multiple_of((shard * GLOBAL_CROPS + crop) * n_img, n_img), n_img), :]
                for crop in range(GLOBAL_CROPS)]
        both = tops[0] + tops[1]
        for view in range(ALL_CROPS):
            rows = pl.ds(base + view * n_img, n_img)
            target = both - tops[view] if view < GLOBAL_CROPS else both
            wide = wide_ref[rows, :]
            soft = exp_u_ref[rows, :] * jnp.concatenate([wide, wide], axis=1)
            g_ref[to_core, pl.ds(land + view * n_img, n_img), :] = (soft - target) * factor
        return carry

    lax.fori_loop(0, shards, combine, 0)
    await_all(n_dev)
    near = pltpu.make_async_remote_copy(
        src_ref=g_ref.at[1 - core], dst_ref=near_recv, send_sem=near_send_sem, recv_sem=near_recv_sem,
        device_id=place_of(chip * 2 + (1 - core), sizes), device_id_type=mesh_type)
    near.start()
    turn_factors(n_img, weight_ref, s_ref, soft_ref, pair_ref)
    get_v.wait()
    get_hi.wait()
    near.wait()
    acc_ref[...] = g_ref[core] + near_recv[...]
    piece = acc_ref.shape[0] // chips
    copies = []
    for step in range(1, chips):
        peer = lax.rem(chip + step, chips)
        copy = pltpu.make_async_remote_copy(
            src_ref=acc_ref.at[pl.ds(pl.multiple_of(peer * piece, n_img), piece)], dst_ref=piece_recv.at[step],
            send_sem=piece_send_sem.at[step], recv_sem=piece_recv_sem.at[step],
            device_id=place_of(peer * 2 + core, sizes), device_id_type=mesh_type)
        copy.start()
        copies.append(copy)
    into_early = functools.partial(grad_block, early_ref, 0)
    lax.fori_loop(0, steps // 2, into_early, 0)
    total = acc_ref[pl.ds(pl.multiple_of(chip * piece, n_img), piece), :]
    for step in range(1, chips):
        copies[step - 1].wait()
        total = total + piece_recv[step]
    piece_ref[...] = total
    copies = []
    for step in range(1, chips):
        peer = lax.rem(chip + step, chips)
        copy = pltpu.make_async_remote_copy(
            src_ref=piece_ref, dst_ref=gathered.at[step], send_sem=all_send_sem.at[step], recv_sem=all_recv_sem.at[step],
            device_id=place_of(peer * 2 + core, sizes), device_id_type=mesh_type)
        copy.start()
        copies.append(copy)
    full_ref[pl.ds(pl.multiple_of(chip * piece, n_img), piece), :] = total
    lax.fori_loop(steps // 2, turn, into_early, 0)
    lax.fori_loop(turn, steps, functools.partial(grad_block, late_ref, turn), 0)
    for step in range(1, chips):
        copies[step - 1].wait()
        owner = lax.rem(chip + chips - step, chips)
        full_ref[pl.ds(pl.multiple_of(owner * piece, n_img), piece), :] = gathered[step]
    for base in range(0, full_ref.shape[0], per_dev):
        for view in range(ALL_CROPS):
            for lane in range(depth // LANES):
                at = pl.ds(lane * LANES, LANES)
                rows = pl.ds(base + view, n_img, stride=ALL_CROPS)
                out_ref[lane, rows, :] = full_ref[pl.ds(base + view * n_img, n_img), at]


def crop_lines(part, s_all, hi_u, lo_u, sizes, n_img):
    lines = (part.shape[0] // LANES // 8 + 1) * 8
    n_dev = 1
    for size in sizes:
        n_dev *= size
    vmem = pl.BlockSpec(memory_space=pltpu.VMEM)
    line = jax.ShapeDtypeStruct((lines, LANES), jnp.float32)
    return pl.pallas_call(
        functools.partial(line_kernel, sizes, n_img), out_shape=(line, line), in_specs=[vmem] * 4, out_specs=(vmem,) * 2,
        scratch_shapes=[
            pltpu.VMEM((lines, LANES), jnp.float32), pltpu.VMEM((n_dev, lines, LANES), jnp.float32),
            pltpu.SemaphoreType.DMA((n_dev,)), pltpu.SemaphoreType.DMA((n_dev,))],
        compiler_params=pltpu.CompilerParams(collective_id=1, has_side_effects=True, vmem_limit_bytes=24 << 20),
        cost_estimate=pl.CostEstimate(flops=5 * 10 ** 9, bytes_accessed=4 << 20, transcendentals=0),
    )(part, s_all, hi_u, lo_u)


def emb_grads(weight, exp_u, hi_u, s_all, exp_lo, hi, protos, sizes, n_img, factor):
    n_student, depth = exp_u.shape
    n_rows, width = hi.shape
    block = 512
    n_dev = 1
    for size in sizes:
        n_dev *= size
    half, chips = n_student // 2, n_dev // 2
    vmem, hbm = pl.BlockSpec(memory_space=pltpu.VMEM), pl.BlockSpec(memory_space=pl.ANY)
    wide, low = jnp.float32, jnp.bfloat16
    dma = pltpu.SemaphoreType.DMA
    return pl.pallas_call(
        functools.partial(emb_kernel, sizes, n_img, factor, block),
        out_shape=(jax.ShapeDtypeStruct((depth // LANES, half, LANES), wide), jax.ShapeDtypeStruct((depth, width - width // 4), wide),
                   jax.ShapeDtypeStruct((depth, width // 4), wide)),
        in_specs=[vmem] * 4 + [hbm] * 3, out_specs=(vmem,) * 3,
        scratch_shapes=[
            pltpu.VMEM((n_student, LANES), wide), pltpu.VMEM((2, half, depth), wide), pltpu.VMEM((half, depth), wide),
            pltpu.VMEM((half, depth), wide), pltpu.VMEM((chips, half // chips, depth), wide),
            pltpu.VMEM((half // chips, depth), wide), pltpu.VMEM((chips, half // chips, depth), wide),
            pltpu.VMEM((half, depth), wide),
            pltpu.VMEM((depth, n_student), low), pltpu.VMEM((depth, n_rows), low),
            pltpu.VMEM((2, n_student, block), low), pltpu.VMEM((n_rows, width), low), pltpu.VMEM((depth, width), low),
            dma, dma, dma((chips,)), dma((chips,)), dma((chips,)), dma((chips,)), dma((2,)), dma, dma],
        compiler_params=pltpu.CompilerParams(collective_id=2, has_side_effects=True, vmem_limit_bytes=56 << 20),
        cost_estimate=pl.CostEstimate(flops=30 * 10 ** 9, bytes_accessed=40 << 20, transcendentals=0),
    )(weight, exp_u, hi_u, s_all, exp_lo, hi, protos)


def place_kernel(src_ref, *refs):
    refs[-1][...] = src_ref[...]


def place_blocks(src, shards, block, total, first, held=None):
    depth, width = src.shape
    count = width // (shards * block)
    stride = total // (shards * block)
    in_specs = [pl.BlockSpec((depth, block), lambda d, j: (0, d * count + j))]
    return pl.pallas_call(
        place_kernel, grid=(shards, count), out_shape=jax.ShapeDtypeStruct((depth, total), src.dtype),
        in_specs=in_specs + [pl.BlockSpec(memory_space=pl.ANY)] * (held is not None),
        out_specs=pl.BlockSpec((depth, block), lambda d, j: (0, d * stride + first + j)),
        input_output_aliases={} if held is None else {1: 0},
        compiler_params=pltpu.CompilerParams(dimension_semantics=('arbitrary', 'arbitrary')),
        cost_estimate=pl.CostEstimate(flops=10 ** 9, bytes_accessed=8 * depth * width, transcendentals=0),
    )(*((src,) if held is None else (src, held)))


def solution(mesh):
    vp_size = mesh.shape['vp']
    dp_size = mesh.shape['dp']
    sizes = (vp_size, dp_size // 4, 2, 2)
    fine = Mesh(mesh.devices.reshape(sizes), AXES)
    data = ('y', 'x', 'core')

    def local_step(student_x, teacher_x, w_in, b_in, w_mid, b_mid, w_out, b_out, protos,
                   ema_w_in, ema_b_in, ema_w_mid, ema_b_mid, ema_w_out, ema_b_out, ema_protos):
        n_img = student_x.shape[0] // ALL_CROPS
        part = protos.shape[1] // dp_size
        n_proto = protos.shape[1] * vp_size
        n_rows = GLOBAL_CROPS * n_img * dp_size
        n_student = ALL_CROPS * n_img * dp_size
        core = lax.axis_index('core')
        data_idx = (lax.axis_index('y') * 2 + lax.axis_index('x')) * 2 + core
        base = data_idx.reshape(1)

        rows_b = (ema_b_in, ema_b_mid, b_in, b_mid, ema_b_out, b_out)
        starts = []
        for row in rows_b:
            starts.append(starts[-1] + width if starts else 0)
            width = row.shape[0]
        total = starts[-1] + width
        biases = sum(jnp.pad(row.astype(jnp.float32), (start, total - start - row.shape[0]))
                     for row, start in zip(rows_b, starts))[None]
        offsets = (starts[0], starts[1], starts[4], starts[2], starts[3], starts[5])
        both = head_pass(teacher_x, student_x, biases, offsets, (ema_w_in, ema_w_mid, ema_w_out), (w_in, w_mid, w_out))
        both = gather_rows(both[None], data)
        both, own_x = lax.optimization_barrier((both, student_x.astype(jnp.float32)))
        half_wide = gather_rows(own_x, ('y', 'x'))

        q_hi, q_lo, q_row, s_all = sinkhorn(both, ema_protos, sizes, n_proto, n_rows, part)
        exp_lo, row_part, exp_u, hi_u, lo_u = soft_pass(base, s_all, protos, q_hi, q_lo)
        scale = 1.0 / (n_img * dp_size * GLOBAL_CROPS * (ALL_CROPS - 1))
        factor = scale / TEMP_STUDENT
        sums, weight = crop_lines(row_part, s_all, hi_u, lo_u, sizes, n_img)
        g_emb, g_early, g_late = emb_grads(weight, exp_u, hi_u, s_all, exp_lo, q_hi, protos, sizes, n_img, factor)
        g_emb = jnp.concatenate([g_emb[lane] for lane in range(g_emb.shape[0])], axis=1)
        g_early, g_late, half_wide = lax.optimization_barrier((g_early, g_late, half_wide))
        all_early = lax.all_gather(g_early, data, axis=1, tiled=True)

        per_view = q_row[:n_rows // LANES].reshape(dp_size, GLOBAL_CROPS, n_img)
        pad = jnp.pad(per_view, ((0, 0), (0, ALL_CROPS - GLOBAL_CROPS), (0, 0)))
        t_row = (jnp.sum(per_view, axis=1, keepdims=True) - pad).reshape(-1)
        row_line = sums.reshape(-1)[:n_student]
        hits = sums[n_student // LANES, 0]
        loss = (jnp.sum(t_row * jnp.log(row_line)) - hits / TEMP_STUDENT) * scale

        hid_one, slope_one, half_x = mlp_layer(half_wide, w_in, biases, offsets[3])
        hid_one, g_late = lax.optimization_barrier((hid_one, g_late))
        all_late = lax.all_gather(g_late, data, axis=1, tiled=True)
        hid_two, slope_two = mlp_layer(hid_one, w_mid, biases, offsets[4])
        grads = mlp_backward(g_emb, half_x, (hid_one, slope_one, hid_two, slope_two), w_mid, w_out, b_out)
        other = lambda g: lax.ppermute(g, 'core', [(0, 1), (1, 0)])
        got_mid, got_in = other(grads[2]), other(grads[0])
        sum_mid = grads[2] + got_mid
        small = jnp.concatenate([grads[1], grads[3], grads[5]])
        small, g_out, sum_mid = lax.optimization_barrier((small, grads[4], sum_mid))
        got_small, got_out = other(small), other(g_out)
        sum_in = grads[0] + got_in
        biases = small + got_small
        sum_out = g_out + got_out
        all_early, sum_in, sum_out, biases = lax.optimization_barrier((all_early, sum_in, sum_out, biases))
        block = part // 4
        g_protos = place_blocks(all_early, dp_size, block, protos.shape[1], 0)
        g_protos = place_blocks(all_late, dp_size, block, protos.shape[1], 3, g_protos)
        b_grads = jnp.split(biases, [b_in.shape[0], b_in.shape[0] + b_mid.shape[0]])
        return (loss, sum_in, b_grads[0], sum_mid, b_grads[1], sum_out, b_grads[2], g_protos)

    by_rows = P(data, None)
    by_cols = P(None, 'vp')
    replicated = P()
    head_specs = (replicated,) * 6
    in_specs = (by_rows, by_rows) + head_specs + (by_cols,) + head_specs + (by_cols,)
    out_specs = (replicated,) * 7 + (by_cols,)
    return jax.shard_map(local_step, mesh=fine, in_specs=in_specs, out_specs=out_specs, check_vma=False)
```
